32 devices in a mesh: dp: 2 (over z, core), ep: 16 (over x, y).
Axes of the slice: x: 4, y: 4, z: 1, core: 2. Of those that a mesh axis runs over, the one named last changes fastest.
The devices are a block of a 4x4x8 slice.
Arguments:
- x: bfloat16 [2, 16, 256, 3072], P('dp', 'ep'), parts along dimension 0
- expert: int32 [2, 16, 256, 4], P('dp', 'ep'), parts along dimension 0
- slot: int32 [2, 16, 256, 4], P('dp', 'ep'), parts along dimension 0
- gate: float32 [2, 16, 256, 4], P('dp', 'ep'), parts along dimension 0
- w_gate: bfloat16 [16, 3072, 10752], P('ep')
- w_up: bfloat16 [16, 3072, 10752], P('ep')
- w_down: bfloat16 [16, 10752, 3072], P('ep')
Outputs:
- y: bfloat16 [2, 16, 256, 3072], P('dp', 'ep'), parts along dimension 0
There are 2 independent parts. The reference program is written for one: setup_inputs(seed, part) draws one part's arguments, and reference() takes and returns one part's arrays. A program takes and returns all parts, laid end to end along the dimension named above; an argument that names none is the same for every part.
All inputs are finite; a program needn't handle non-finite values.
Results may differ from the reference program's by a relative error of at most 0.009.
Values are sent between devices in bfloat16 or wider.
A program may use at most 768 MiB of HBM per device.

```python
import jax
import jax.numpy as jnp

MEMBERS = 16
TOKENS = 256
D = 3072
FF = 10752
TOP = 4
EXPERTS = 16
SLOTS = 5 * TOKENS * TOP // (4 * EXPERTS)


def setup_inputs(seed: int = 0, part: int = 0) -> dict:
    own, k1, k2, k3, k4, k5, k6 = jax.random.split(jax.random.key(seed), 7)
    kx, ke, kl, kg = jax.random.split(jax.random.fold_in(own, part), 4)
    devices = (1, MEMBERS)
    place = jax.random.permutation(kl, jnp.arange(EXPERTS, dtype=jnp.uint32))
    slow = ((EXPERTS + (9 * place) % EXPERTS) << ((9 * place) // EXPERTS)) // EXPERTS
    wait = (jax.random.bits(ke, (*devices, TOKENS, EXPERTS), jnp.uint32) >> 10) * slow
    expert = jnp.argsort(wait, axis=-1)[..., :TOP].astype(jnp.int32)
    chosen = jax.nn.one_hot(expert, EXPERTS, dtype=jnp.int32)
    in_line = jnp.cumsum(chosen.reshape(*devices, TOKENS * TOP, EXPERTS), axis=2) - 1
    slot = jnp.sum(in_line.reshape(chosen.shape) * chosen, axis=-1)

    def one(key, rows, columns):
        return (jax.random.normal(key, (rows, columns), jnp.float32) * rows**-0.5).astype(jnp.bfloat16)

    def weights(key, rows, columns):
        return jax.lax.map(lambda k: one(k, rows, columns), jax.random.split(key, EXPERTS))

    return {
        "x": jax.random.normal(kx, (*devices, TOKENS, D), jnp.float32).astype(jnp.bfloat16),
        "expert": expert,
        "slot": slot,
        "gate": jax.nn.softmax(jax.random.normal(kg, expert.shape, jnp.float32)),
        "w_gate": weights(k1, D, FF),
        "w_up": weights(k2, D, FF),
        "w_down": weights(k3, FF, D),
    }


def einsum(form, a, b):
    return jnp.einsum(form, a.astype(jnp.float32), b.astype(jnp.float32))


def reference(x, expert, slot, gate, w_gate, w_up, w_down):
    to_expert = jax.nn.one_hot(expert, EXPERTS, dtype=jnp.bfloat16)
    to_slot = jax.nn.one_hot(slot, SLOTS, dtype=jnp.bfloat16)
    weighted = to_expert * gate[..., None].astype(jnp.bfloat16)
    dispatch = einsum("abtke,abtkc->abtec", to_expert, to_slot).astype(jnp.bfloat16)
    combine = einsum("abtke,abtkc->abtec", weighted, to_slot).astype(jnp.bfloat16)
    z = einsum("abtec,abtd->aebcd", dispatch, x).astype(jnp.bfloat16)
    h = jax.nn.silu(einsum("aebcd,edf->aebcf", z, w_gate))
    h = (h * einsum("aebcd,edf->aebcf", z, w_up)).astype(jnp.bfloat16)
    out = einsum("aebcf,efd->aebcd", h, w_down).astype(jnp.bfloat16)
    y = einsum("abtec,aebcd->abtd", combine, out)
    return y.astype(jnp.bfloat16)
```

```python
import functools
import math

import jax
import jax.numpy as jnp
from jax import lax
from jax.experimental import pallas as pl
from jax.experimental.pallas import tpu as pltpu
from jax.sharding import PartitionSpec as P

MESH = pl.DeviceIdType.MESH
F32, BF16 = jnp.float32, jnp.bfloat16
COLS = 256
PAIRS = 2
RING = 3


def plan(side):
    far = lambda v: min(v, side - v)
    peers = sorted(((far(a) + far(b), a, b) for a in range(side) for b in range(side)))
    near = [(a, b) for n, a, b in peers if n <= 1]
    mid = [(a, b) for n, a, b in peers if n == 2]
    rest = [(a, b) for n, a, b in peers if n > 2]
    return near, mid, rest


def kernel(
    side, slots, x_ref, expert_ref, slot_ref, gate_ref, wg_ref, wu_ref, wd_ref, y_ref,
    z, h, back, w, comb, x_sem, w_sem, y_sem, out_s, out_r, far_s, far_r, end_s, end_r,
):
    tokens, d = x_ref.shape
    ff = wd_ref.shape[0]
    near, mid, rest = plan(side)
    order = near + mid + rest
    where = {o: p for p, o in enumerate(order)}
    mirror = [where[(-a) % side, (-b) % side] for a, b in order]
    members = len(order)
    n_near, n_end = len(near), len(near) + len(mid)
    rows = lambda lo, hi: pl.ds(lo * slots, (hi - lo) * slots)
    me = lax.axis_index("ep")
    my_x, my_y = me // side, lax.rem(me, side)

    def device(p):
        a, b = order[p]
        return {"ep": lax.rem(my_x + a, side) * side + lax.rem(my_y + b, side)}

    barrier = pltpu.get_barrier_semaphore()
    for p in range(1, members):
        pl.semaphore_signal(barrier, inc=1, device_id=device(p), device_id_type=MESH)

    x_at = h.at[pl.ds(n_near * slots, tokens), pl.ds(d, d)]
    x_copy = pltpu.make_async_copy(x_ref, x_at, x_sem)
    x_copy.start()

    def staged(p):
        if p < n_near:
            return h.at[rows(n_near + p - 1, n_near + p), pl.ds(2 * d, d)]
        return h.at[rows(p, p + 1), pl.ds(0, d)]

    n_up, n_down = ff // (COLS * PAIRS), d // COLS
    steps = [n_up, n_up, n_down, n_up, n_down]

    def tile_up(i, s):
        for k in range(PAIRS):
            at = pl.ds(pl.multiple_of((i * PAIRS + k) * COLS, COLS), COLS)
            pltpu.make_async_copy(wg_ref.at[:, at], w.at[s, pl.ds(2 * k * d, d)], w_sem.at[s]).start()
            pltpu.make_async_copy(wu_ref.at[:, at], w.at[s, pl.ds((2 * k + 1) * d, d)], w_sem.at[s]).start()

    def tile_down(i, s):
        at = pl.ds(pl.multiple_of(i * COLS, COLS), COLS)
        pltpu.make_async_copy(wd_ref.at[:, at], w.at[s, pl.ds(0, ff)], w_sem.at[s]).start()

    fetch = [tile_up, tile_up, tile_down, tile_up, tile_down]
    taken = [2 * PAIRS * d, 2 * PAIRS * d, ff, 2 * PAIRS * d, ff]
    for i in range(RING - 1):
        tile_up(i, i)

    def phase(k, lo, hi, body):
        n, first = steps[k], sum(steps[:k])

        def step(i, carry):
            s = lax.rem(i + first, RING)
            got = w.at[s, pl.ds(0, taken[k])]
            pltpu.make_async_copy(got, got, w_sem.at[s]).wait()
            ahead = i + RING - 1
            s_ahead = lax.rem(ahead + first, RING)

            @pl.when(ahead < n)
            def _():
                fetch[k](ahead, s_ahead)

            if k + 1 < len(steps):

                @pl.when(ahead >= n)
                def _():
                    fetch[k + 1](ahead - n, s_ahead)

            body(i, s)
            return carry

        lax.fori_loop(lo, hi, step, 0)

    expert, slot = expert_ref[...], slot_ref[...]
    off = lax.rem(expert // side - my_x + side, side) * side + lax.rem(lax.rem(expert, side) - my_y + side, side)
    place = jnp.zeros_like(off)
    for p, (a, b) in enumerate(order):
        place = jnp.where(off == a * side + b, p, place)
    code = jnp.where(slot < slots, place * slots + slot, -1)
    gate = gate_ref[...].astype(BF16).astype(F32)

    def chosen(lo, n, value):
        row = lax.broadcasted_iota(jnp.int32, (n, tokens), 0) + lo
        out = jnp.zeros((n, tokens), F32)
        for j in range(code.shape[0]):
            out = jnp.where(row == code[j : j + 1, :], value(j), out)
        return out

    def block_rows(lo, hi, at):
        pick = chosen(lo * slots, (hi - lo) * slots, lambda j: 1.0).astype(BF16)
        for c in range(0, d, 2 * COLS):
            cols = pl.ds(c, min(2 * COLS, d - c))
            got = jnp.dot(pick, x_at[:, cols], preferred_element_type=F32).astype(BF16)
            for p in range(lo, hi):
                at(p)[:, cols] = got[(p - lo) * slots : (p - lo + 1) * slots]

    def send(p):
        return pltpu.make_async_remote_copy(
            src_ref=staged(p),
            dst_ref=z.at[rows(mirror[p], mirror[p] + 1)],
            send_sem=out_s.at[p],
            recv_sem=out_r.at[mirror[p]],
            device_id=device(p),
            device_id_type=MESH,
        )

    def arrived(lo, hi):
        for p in range(lo, hi):
            got = z.at[rows(p, p + 1)]
            pltpu.make_async_copy(got, got, out_r.at[p]).wait()

    x_copy.wait()
    block_rows(1, n_near, staged)
    pl.semaphore_wait(barrier, members - 1)
    for p in range(1, n_near):
        send(p).start()
    block_rows(n_end, members, staged)
    for p in range(n_end, members):
        send(p).start()
    block_rows(n_near, n_end, staged)
    for p in range(n_near, n_end):
        send(p).start()
    block_rows(0, 1, lambda p: z.at[rows(0, 1)])
    for c in range(0, members * slots, 128):
        part = chosen(c, 128, lambda j: gate[j : j + 1, :])
        comb[:, pl.ds(c, 128)] = part.T.astype(BF16)

    def up(lo, hi):
        at = rows(lo, hi)

        def body(i, s):
            for k in range(PAIRS):
                g = jnp.dot(z[at, :], w[s, pl.ds(2 * k * d, d)], preferred_element_type=F32)
                u = jnp.dot(z[at, :], w[s, pl.ds((2 * k + 1) * d, d)], preferred_element_type=F32)
                cols = pl.ds(pl.multiple_of((i * PAIRS + k) * COLS, COLS), COLS)
                h[at, cols] = (jax.nn.silu(g) * u).astype(BF16)

        return body

    def result(p, c, send_sem, recv_sem):
        cols = pl.ds(pl.multiple_of(c * COLS, COLS), COLS)
        return pltpu.make_async_remote_copy(
            src_ref=z.at[rows(p, p + 1), cols],
            dst_ref=back.at[rows(mirror[p], mirror[p] + 1), cols],
            send_sem=send_sem,
            recv_sem=recv_sem,
            device_id=device(p),
            device_id_type=MESH,
        )

    def down_rest(i, s):
        at = rows(n_end, members)
        cols = pl.ds(pl.multiple_of(i * COLS, COLS), COLS)
        out = jnp.dot(h[at, :], w[s, pl.ds(0, ff)], preferred_element_type=F32)
        z[at, cols] = out.astype(BF16)
        for p in range(n_end, members):
            result(p, i, far_s, far_r).start()

    def down_end(i, s):
        cols = pl.ds(pl.multiple_of(i * COLS, COLS), COLS)
        out = jnp.dot(h[rows(0, n_end), :], w[s, pl.ds(0, ff)], preferred_element_type=F32).astype(BF16)
        back[rows(0, 1), cols] = out[:slots]
        z[rows(1, n_end), cols] = out[slots:]
        for p in range(n_near, n_end):
            result(p, i, end_s, end_r.at[i]).start()
        for p in range(1, n_near):
            result(p, i, end_s, end_r.at[i]).start()

    arrived(1, n_near)
    phase(0, 0, n_up, up(0, n_near))
    arrived(n_end, members)
    for p in range(n_end, members):
        send(p).wait_send()
    phase(1, 0, n_up, up(n_end, members))
    phase(2, 0, n_down, down_rest)
    arrived(n_near, n_end)
    for p in range(1, n_end):
        send(p).wait_send()
    phase(3, 0, n_up, up(n_near, n_end))
    phase(4, 0, n_down, down_end)

    got = back.at[rows(n_end, members)]
    pltpu.make_async_copy(got, got, far_r).wait()
    writes = []
    for c in range(n_down):
        cols = pl.ds(c * COLS, COLS)
        got = back.at[rows(1, n_end), cols]
        pltpu.make_async_copy(got, got, end_r.at[c]).wait()
        total = jnp.dot(comb[...], back[:, cols], preferred_element_type=F32)
        kept = w.at[0, pl.ds(c * tokens, tokens)]
        kept[...] = total.astype(BF16)
        write = pltpu.make_async_copy(kept, y_ref.at[:, cols], y_sem)
        write.start()
        writes.append(write)
    for write in writes:
        write.wait()
    gone = z.at[rows(n_end, members)]
    pltpu.make_async_copy(gone, gone, far_s).wait()
    gone = z.at[rows(1, n_end)]
    pltpu.make_async_copy(gone, gone, end_s).wait()


def solution(mesh):
    members = mesh.shape["ep"]
    side = math.isqrt(members)

    def layer(x, expert, slot, gate, w_gate, w_up, w_down):
        tokens, d = x.shape[2:]
        ff, top = w_gate.shape[2], expert.shape[3]
        slots = 5 * tokens * top // (4 * members)
        total = members * slots
        any_ = pl.BlockSpec(memory_space=pl.ANY)
        vmem = pl.BlockSpec(memory_space=pltpu.VMEM)
        turned = lambda v: v.reshape(tokens, top).T
        y = pl.pallas_call(
            functools.partial(kernel, side, slots),
            out_shape=jax.ShapeDtypeStruct((tokens, d), BF16),
            in_specs=[any_, vmem, vmem, vmem, any_, any_, any_],
            out_specs=any_,
            scratch_shapes=[
                pltpu.VMEM((total, d), BF16),
                pltpu.VMEM((total, ff), BF16),
                pltpu.VMEM((total, d), BF16),
                pltpu.VMEM((RING, max(2 * PAIRS * d, ff), COLS), BF16),
                pltpu.VMEM((tokens, total), BF16),
                pltpu.SemaphoreType.DMA,
                pltpu.SemaphoreType.DMA((RING,)),
                pltpu.SemaphoreType.DMA,
                pltpu.SemaphoreType.DMA((members,)),
                pltpu.SemaphoreType.DMA((members,)),
                pltpu.SemaphoreType.DMA,
                pltpu.SemaphoreType.DMA,
                pltpu.SemaphoreType.DMA,
                pltpu.SemaphoreType.DMA((d // COLS,)),
            ],
            compiler_params=pltpu.CompilerParams(
                collective_id=0, has_side_effects=True, vmem_limit_bytes=67_043_328
            ),
            name="moe",
        )(
            x.reshape(tokens, d), turned(expert), turned(slot), turned(gate),
            w_gate.reshape(d, ff), w_up.reshape(d, ff), w_down.reshape(ff, d),
        )
        return y.reshape(1, 1, tokens, d)

    per_device, per_expert = P("dp", "ep", None, None), P("ep", None, None)
    return jax.shard_map(
        layer,
        mesh=mesh,
        in_specs=(per_device,) * 4 + (per_expert,) * 3,
        out_specs=per_device,
        check_vma=False,
    )
```

```python
import functools
import math

import jax
import jax.numpy as jnp
from jax import lax
from jax.experimental import pallas as pl
from jax.experimental.pallas import tpu as pltpu
from jax.sharding import PartitionSpec as P

MESH = pl.DeviceIdType.MESH
F32, BF16 = jnp.float32, jnp.bfloat16
COLS = 256
PAIRS = 2
RING = 3
LAG = 4


def plan(side):
    far = lambda v: min(v, side - v)
    peers = sorted(((far(a) + far(b), a, b) for a in range(side) for b in range(side)))
    near = [(a, b) for n, a, b in peers if n <= 1]
    mid = [(a, b) for n, a, b in peers if n == 2]
    mid.sort(key=lambda o: (2 * o[0] == side, o[0], o[1] if o[0] == 1 else -o[1]))
    rest = [(a, b) for n, a, b in peers if n > 2]
    rest.sort(key=lambda o: (-far(o[0]) - far(o[1]), -far(o[0])))
    return near, mid, rest


def kernel(
    side, slots, x_ref, expert_ref, slot_ref, gate_ref, wg_ref, wu_ref, wd_ref, y_ref,
    z, h, back, w, comb, x_sem, w_sem, y_sem, out_s, out_r, far_s, far_r, mid_s, mid_r, near_s, near_r,
):
    tokens, d = x_ref.shape
    ff = wd_ref.shape[0]
    near, mid, rest = plan(side)
    order = near + mid + rest
    where = {o: p for p, o in enumerate(order)}
    mirror = [where[(-a) % side, (-b) % side] for a, b in order]
    members = len(order)
    n_near, n_end = len(near), len(near) + len(mid)
    rows = lambda lo, hi: pl.ds(lo * slots, (hi - lo) * slots)
    me = lax.axis_index("ep")
    my_x, my_y = me // side, lax.rem(me, side)

    def device(p):
        a, b = order[p]
        return {"ep": lax.rem(my_x + a, side) * side + lax.rem(my_y + b, side)}

    barrier = pltpu.get_barrier_semaphore()
    for p in range(1, members):
        pl.semaphore_signal(barrier, inc=1, device_id=device(p), device_id_type=MESH)

    x_at = h.at[pl.ds(n_near * slots, tokens), pl.ds(d, d)]
    x_copy = pltpu.make_async_copy(x_ref, x_at, x_sem)
    x_copy.start()

    def staged(p):
        if p < n_near:
            return h.at[rows(n_near + p - 1, n_near + p), pl.ds(2 * d, d)]
        return h.at[rows(p, p + 1), pl.ds(0, d)]

    n_up, n_down = ff // (COLS * PAIRS), d // COLS
    steps = [n_up, n_up, n_down, n_up, n_down, n_down]

    def tile_up(i, s):
        for k in range(PAIRS):
            at = pl.ds(pl.multiple_of((i * PAIRS + k) * COLS, COLS), COLS)
            pltpu.make_async_copy(wg_ref.at[:, at], w.at[s, pl.ds(2 * k * d, d)], w_sem.at[s]).start()
            pltpu.make_async_copy(wu_ref.at[:, at], w.at[s, pl.ds((2 * k + 1) * d, d)], w_sem.at[s]).start()

    def tile_down(i, s):
        at = pl.ds(pl.multiple_of(i * COLS, COLS), COLS)
        pltpu.make_async_copy(wd_ref.at[:, at], w.at[s, pl.ds(0, ff)], w_sem.at[s]).start()

    fetch = [tile_up, tile_up, tile_down, tile_up, tile_down, tile_down]
    taken = [2 * PAIRS * d, 2 * PAIRS * d, ff, 2 * PAIRS * d, ff, ff]
    def phase(k, lo, hi, body):
        n, first = steps[k], sum(steps[:k])

        def step(i, carry):
            s = lax.rem(i + first, RING)
            got = w.at[s, pl.ds(0, taken[k])]
            with jax.named_scope(f"weights{k}"):
                pltpu.make_async_copy(got, got, w_sem.at[s]).wait()
            ahead = i + RING - 1
            s_ahead = lax.rem(ahead + first, RING)

            @pl.when(ahead < n)
            def _():
                fetch[k](ahead, s_ahead)

            if k + 1 < len(steps):

                @pl.when(ahead >= n)
                def _():
                    fetch[k + 1](ahead - n, s_ahead)

            with jax.named_scope(f"body{k}"):
                body(i, s)
            return carry

        lax.fori_loop(lo, hi, step, 0)

    expert, slot = expert_ref[...], slot_ref[...]
    off = lax.rem(expert // side - my_x + side, side) * side + lax.rem(lax.rem(expert, side) - my_y + side, side)
    place = jnp.zeros_like(off)
    for p, (a, b) in enumerate(order):
        place = jnp.where(off == a * side + b, p, place)
    code = jnp.where(slot < slots, place * slots + slot, -1)
    gate = gate_ref[...].astype(BF16).astype(F32)

    def chosen(lo, n, value):
        row = lax.broadcasted_iota(jnp.int32, (n, tokens), 0) + lo
        out = jnp.zeros((n, tokens), F32)
        for j in range(code.shape[0]):
            out = jnp.where(row == code[j : j + 1, :], value(j), out)
        return out

    def block_rows(lo, hi, at):
        pick = chosen(lo * slots, (hi - lo) * slots, lambda j: 1.0).astype(BF16)
        for c in range(0, d, 2 * COLS):
            cols = pl.ds(c, min(2 * COLS, d - c))
            got = jnp.dot(pick, x_at[:, cols], preferred_element_type=F32).astype(BF16)
            for p in range(lo, hi):
                at(p)[:, cols] = got[(p - lo) * slots : (p - lo + 1) * slots]

    def send(p):
        return pltpu.make_async_remote_copy(
            src_ref=staged(p),
            dst_ref=z.at[rows(mirror[p], mirror[p] + 1)],
            send_sem=out_s.at[p],
            recv_sem=out_r.at[mirror[p]],
            device_id=device(p),
            device_id_type=MESH,
        )

    def arrived(lo, hi):
        for p in range(lo, hi):
            got = z.at[rows(p, p + 1)]
            with jax.named_scope(f"arrive{p}"):
                pltpu.make_async_copy(got, got, out_r.at[p]).wait()

    with jax.named_scope("x"):
        x_copy.wait()
    for i in range(RING - 1):
        tile_up(i, i)
    block_rows(1, n_near, staged)
    with jax.named_scope("barrier"):
        pl.semaphore_wait(barrier, members - 1)
    for p in range(1, n_near):
        send(p).start()
    with jax.named_scope("rows"):
        block_rows(n_end, members, staged)
        block_rows(n_near, n_end, staged)
        block_rows(0, 1, lambda p: z.at[rows(0, 1)])
    for c in range(0, members * slots, 128):
        part = chosen(c, 128, lambda j: gate[j : j + 1, :])
        comb[:, pl.ds(c, 128)] = part.T.astype(BF16)

    def up(lo, hi):
        at = rows(lo, hi)

        def body(i, s):
            for k in range(PAIRS):
                g = jnp.dot(z[at, :], w[s, pl.ds(2 * k * d, d)], preferred_element_type=F32)
                u = jnp.dot(z[at, :], w[s, pl.ds((2 * k + 1) * d, d)], preferred_element_type=F32)
                cols = pl.ds(pl.multiple_of((i * PAIRS + k) * COLS, COLS), COLS)
                h[at, cols] = (jax.nn.silu(g) * u).astype(BF16)

        return body

    def result(p, c, n, send_sem, recv_sem):
        cols = pl.ds(pl.multiple_of(c * COLS, COLS), n * COLS)
        return pltpu.make_async_remote_copy(
            src_ref=z.at[rows(p, p + 1), cols],
            dst_ref=back.at[rows(mirror[p], mirror[p] + 1), cols],
            send_sem=send_sem,
            recv_sem=recv_sem,
            device_id=device(p),
            device_id_type=MESH,
        )

    def send_results(lo, hi, c, n, piece, send_sem, recv_sem):
        for p in range(lo, hi):
            result(p, c, n, send_sem, recv_sem.at[piece]).start()

    def results_arrived(lo, hi, c, n, piece, recv_sem, name):
        got = back.at[rows(lo, hi), pl.ds(pl.multiple_of(c * COLS, COLS), n * COLS)]
        with jax.named_scope(name):
            pltpu.make_async_copy(got, got, recv_sem.at[piece]).wait()

    def down(lo, hi):
        at = rows(lo, hi)

        def body(i, s):
            out = jnp.dot(h[at, :], w[s, pl.ds(0, ff)], preferred_element_type=F32)
            z[at, pl.ds(pl.multiple_of(i * COLS, COLS), COLS)] = out.astype(BF16)

        return body

    def down_near(i, s):
        cols = pl.ds(pl.multiple_of(i * COLS, COLS), COLS)
        out = jnp.dot(h[rows(0, n_near), :], w[s, pl.ds(0, ff)], preferred_element_type=F32).astype(BF16)
        back[rows(0, 1), cols] = out[:slots]
        z[rows(1, n_near), cols] = out[slots:]

    def write(c):
        cols = pl.ds(pl.multiple_of(c * COLS, COLS), COLS)
        return pltpu.make_async_copy(back.at[pl.ds(0, tokens), cols], y_ref.at[:, cols], y_sem)

    def add_up(c):
        cols = pl.ds(pl.multiple_of(c * COLS, COLS), COLS)
        total = jnp.dot(comb[...], back[:, cols], preferred_element_type=F32)
        back[pl.ds(0, tokens), cols] = total.astype(BF16)

    def near_and_add(i, s):
        add_up(i - LAG)
        down_near(i, s)
        write(i - LAG).start()

    arrived(1, n_near)
    for p in range(n_end, members):
        send(p).start()
    phase(0, 0, n_up, up(0, n_near))
    arrived(n_end, members)
    for p in range(n_near, n_end):
        send(p).start()
    for p in range(n_end, members):
        with jax.named_scope("sent_rest"):
            send(p).wait_send()
    phase(1, 0, n_up, up(n_end, members))
    phase(2, 0, n_down, down(n_end, members))
    for p in range(n_end, members):
        result(p, 0, n_down, far_s, far_r).start()
    arrived(n_near, n_end)
    with jax.named_scope("sent_mid"):
        for p in range(1, n_end):
            send(p).wait_send()
    phase(3, 0, n_up, up(n_near, n_end))

    def mid_pair(q, carry):
        phase(4, 2 * q, 2 * q + 2, down(n_near, n_end))
        send_results(n_near, n_end, 2 * q, 2, q, mid_s, mid_r)
        return carry

    lax.fori_loop(0, n_down // 2, mid_pair, 0)

    pairs = (n_down - 2) // 2

    def near_pair(q, carry):
        phase(5, 2 * q, 2 * q + 2, down_near)
        send_results(1, n_near, 2 * q, 2, q, near_s, near_r)
        return carry

    def pair_arrived(q):
        results_arrived(n_near, n_end, 2 * q, 2, q, mid_r, "mid")
        results_arrived(1, n_near, 2 * q, 2, q, near_r, "near")

    def near_pair_and_add(q, carry):
        pair_arrived(q - LAG // 2)
        phase(5, 2 * q, 2 * q + 2, near_and_add)
        send_results(1, n_near, 2 * q, 2, q, near_s, near_r)
        return carry

    lax.fori_loop(0, LAG // 2, near_pair, 0)
    got = back.at[rows(n_end, members)]
    with jax.named_scope("far"):
        pltpu.make_async_copy(got, got, far_r).wait()
    lax.fori_loop(LAG // 2, pairs, near_pair_and_add, 0)
    pair_arrived(pairs - LAG // 2)

    def last(i, s):
        near_and_add(i, s)
        send_results(1, n_near, i, 1, i - pairs, near_s, near_r)

    phase(5, 2 * pairs, n_down, last)
    for q in range(pairs + 1 - LAG // 2, pairs):
        pair_arrived(q)
        add_up(2 * q)
        add_up(2 * q + 1)
        write(2 * q).start()
        write(2 * q + 1).start()
    results_arrived(n_near, n_end, 2 * pairs, 2, pairs, mid_r, "mid")
    for c in range(2 * pairs, n_down):
        results_arrived(1, n_near, c, 1, c - pairs, near_r, "near")
        add_up(c)
        write(c).start()
    with jax.named_scope("written"):
        for c in range(n_down):
            write(c).wait()
    gone = z.at[rows(n_end, members)]
    pltpu.make_async_copy(gone, gone, far_s).wait()
    gone = z.at[rows(n_near, n_end)]
    pltpu.make_async_copy(gone, gone, mid_s).wait()
    gone = z.at[rows(1, n_near)]
    pltpu.make_async_copy(gone, gone, near_s).wait()


def solution(mesh):
    members = mesh.shape["ep"]
    side = math.isqrt(members)

    def layer(x, expert, slot, gate, w_gate, w_up, w_down):
        tokens, d = x.shape[2:]
        ff, top = w_gate.shape[2], expert.shape[3]
        slots = 5 * tokens * top // (4 * members)
        total = members * slots
        any_ = pl.BlockSpec(memory_space=pl.ANY)
        vmem = pl.BlockSpec(memory_space=pltpu.VMEM)
        turned = lambda v: v.reshape(tokens, top).T
        y = pl.pallas_call(
            functools.partial(kernel, side, slots),
            out_shape=jax.ShapeDtypeStruct((tokens, d), BF16),
            in_specs=[any_, vmem, vmem, vmem, any_, any_, any_],
            out_specs=any_,
            scratch_shapes=[
                pltpu.VMEM((total, d), BF16),
                pltpu.VMEM((total, ff), BF16),
                pltpu.VMEM((total, d), BF16),
                pltpu.VMEM((RING, max(2 * PAIRS * d, ff), COLS), BF16),
                pltpu.VMEM((tokens, total), BF16),
                pltpu.SemaphoreType.DMA,
                pltpu.SemaphoreType.DMA((RING,)),
                pltpu.SemaphoreType.DMA,
                pltpu.SemaphoreType.DMA((members,)),
                pltpu.SemaphoreType.DMA((members,)),
                pltpu.SemaphoreType.DMA,
                pltpu.SemaphoreType.DMA,
                pltpu.SemaphoreType.DMA,
                pltpu.SemaphoreType.DMA((d // COLS,)),
                pltpu.SemaphoreType.DMA,
                pltpu.SemaphoreType.DMA((d // COLS,)),
            ],
            compiler_params=pltpu.CompilerParams(
                collective_id=0, has_side_effects=True, vmem_limit_bytes=67_043_328
            ),
            name="moe",
        )(
            x.reshape(tokens, d), turned(expert), turned(slot), turned(gate),
            w_gate.reshape(d, ff), w_up.reshape(d, ff), w_down.reshape(ff, d),
        )
        return y.reshape(1, 1, tokens, d)

    per_device, per_expert = P("dp", "ep", None, None), P("ep", None, None)
    return jax.shard_map(
        layer,
        mesh=mesh,
        in_specs=(per_device,) * 4 + (per_expert,) * 3,
        out_specs=per_device,
        check_vma=False,
    )
```

```python
import functools
import math

import jax
import jax.numpy as jnp
from jax import lax
from jax.experimental import pallas as pl
from jax.experimental.pallas import tpu as pltpu
from jax.sharding import PartitionSpec as P

MESH = pl.DeviceIdType.MESH
F32, BF16 = jnp.float32, jnp.bfloat16
COLS = 256
HELD = 6
OWN = 12
LAG = 6


def plan(side):
    far = lambda v: min(v, side - v)
    peers = sorted(((far(a) + far(b), a, b) for a in range(side) for b in range(side)))
    near = [(a, b) for n, a, b in peers if n <= 1]
    mid = [(a, b) for n, a, b in peers if n == 2]
    mid.sort(key=lambda o: (2 * o[0] == side, o[0], o[1] if o[0] == 1 else -o[1]))
    rest = [(a, b) for n, a, b in peers if n > 2]
    rest.sort(key=lambda o: (-far(o[0]) - far(o[1]), -far(o[0])))
    return near, mid, rest


def kernel(
    side, slots, x_ref, expert_ref, slot_ref, gate_ref, wg_ref, wu_ref, wd_ref, y_ref,
    z, h, back, w, comb, x_sem, w_sem, y_sem, out_s, out_r, far_s, far_r, mid_s, mid_r, near_s, near_r,
):
    tokens, d = x_ref.shape
    ff = wd_ref.shape[0]
    near, mid, rest = plan(side)
    order = near + mid + rest
    where = {o: p for p, o in enumerate(order)}
    mirror = [where[(-a) % side, (-b) % side] for a, b in order]
    members = len(order)
    n_near, n_end = len(near), len(near) + len(mid)
    rows = lambda lo, hi: pl.ds(lo * slots, (hi - lo) * slots)
    me = lax.axis_index("ep")
    my_x, my_y = me // side, lax.rem(me, side)

    def device(p):
        a, b = order[p]
        return {"ep": lax.rem(my_x + a, side) * side + lax.rem(my_y + b, side)}

    x_at = h.at[pl.ds(n_near * slots, tokens), pl.ds(d, d)]
    x_copy = pltpu.make_async_copy(x_ref, x_at, x_sem)
    x_copy.start()

    barrier = pltpu.get_barrier_semaphore()
    for p in range(1, members):
        pl.semaphore_signal(barrier, inc=1, device_id=device(p), device_id_type=MESH)

    def staged(p):
        if p < n_near:
            return h.at[rows(n_near + p - 1, n_near + p), pl.ds(2 * d, d)]
        return h.at[rows(p, p + 1), pl.ds(0, d)]

    n_up, n_down = ff // COLS, d // COLS

    def fetch_up(tile, place):
        at = pl.ds(pl.multiple_of(tile * COLS, COLS), COLS)
        for q, ref in enumerate((wg_ref, wu_ref)):
            to = w.at[pl.ds(pl.multiple_of((2 * place + q) * d, COLS), d)]
            pltpu.make_async_copy(ref.at[:, at], to, w_sem.at[place]).start()

    def fetch_down(tile, place):
        at = pl.ds(pl.multiple_of(tile * COLS, COLS), COLS)
        to = w.at[pl.ds(pl.multiple_of(4 * place * d, COLS), ff)]
        pltpu.make_async_copy(wd_ref.at[:, at], to, w_sem.at[2 * place]).start()

    def fetched(place, n):
        got = w.at[pl.ds(pl.multiple_of(2 * place * d, COLS), n)]
        with jax.named_scope("weights"):
            pltpu.make_async_copy(got, got, w_sem.at[place]).wait()

    def loop(lo, hi, body):
        def step(i, carry):
            body(i)
            return carry

        lax.fori_loop(lo, hi, step, 0)

    expert, slot = expert_ref[...], slot_ref[...]
    off = lax.rem(expert // side - my_x + side, side) * side + lax.rem(lax.rem(expert, side) - my_y + side, side)
    place = jnp.zeros_like(off)
    for p, (a, b) in enumerate(order):
        place = jnp.where(off == a * side + b, p, place)
    code = jnp.where(slot < slots, place * slots + slot, -1)
    gate = gate_ref[...].astype(BF16).astype(F32)

    def chosen(lo, n, value):
        row = lax.broadcasted_iota(jnp.int32, (n, tokens), 0) + lo
        out = jnp.zeros((n, tokens), F32)
        for j in range(code.shape[0]):
            out = jnp.where(row == code[j : j + 1, :], value(j), out)
        return out

    def block_rows(lo, hi, at):
        pick = chosen(lo * slots, (hi - lo) * slots, lambda j: 1.0).astype(BF16)
        for c in range(0, d, 2 * COLS):
            cols = pl.ds(c, min(2 * COLS, d - c))
            got = jnp.dot(pick, x_at[:, cols], preferred_element_type=F32).astype(BF16)
            for p in range(lo, hi):
                at(p)[:, cols] = got[(p - lo) * slots : (p - lo + 1) * slots]

    def send(p):
        return pltpu.make_async_remote_copy(
            src_ref=staged(p),
            dst_ref=z.at[rows(mirror[p], mirror[p] + 1)],
            send_sem=out_s.at[p],
            recv_sem=out_r.at[mirror[p]],
            device_id=device(p),
            device_id_type=MESH,
        )

    def arrived(lo, hi):
        for p in range(lo, hi):
            got = z.at[rows(p, p + 1)]
            with jax.named_scope(f"arrive{p}"):
                pltpu.make_async_copy(got, got, out_r.at[p]).wait()

    with jax.named_scope("x"):
        x_copy.wait()
    for i in range(HELD - 1):
        fetch_up(i, i)
    block_rows(1, n_near, staged)
    with jax.named_scope("barrier"):
        pl.semaphore_wait(barrier, members - 1)
    for p in range(1, n_near):
        send(p).start()
    with jax.named_scope("rows"):
        block_rows(n_end, members, staged)
        block_rows(n_near, n_end, staged)
        block_rows(0, 1, lambda p: z.at[rows(0, 1)])
    for c in range(0, members * slots, 128):
        part = chosen(c, 128, lambda j: gate[j : j + 1, :])
        comb[:, pl.ds(c, 128)] = part.T.astype(BF16)

    def up(lo, hi, tile, place, n):
        at = rows(lo, hi)
        for k in range(n):
            start = [pl.multiple_of((2 * (place + k) + q) * d, COLS) for q in range(2)]
            g = jnp.dot(z[at, :], w[pl.ds(start[0], d), :], preferred_element_type=F32)
            u = jnp.dot(z[at, :], w[pl.ds(start[1], d), :], preferred_element_type=F32)
            cols = pl.ds(pl.multiple_of((tile + k) * COLS, COLS), COLS)
            h[at, cols] = (jax.nn.silu(g) * u).astype(BF16)

    def own_step(j):
        place = j - jnp.where(j >= HELD, HELD, 0)
        fetched(place, 2 * d)
        later = j + HELD - 1

        @pl.when(later < OWN)
        def _():
            fetch_up(later, later - jnp.where(later >= HELD, HELD, 0))

        with jax.named_scope("own"):
            up(0, 1, j, place, 1)

    def thirds(lo, hi, body):
        def outer(o, carry):
            loop(0, 3, lambda r: body(3 * o + r, r, jnp.where(r == 0, 2, r - 1)))
            return carry

        lax.fori_loop(lo // 3, hi // 3, outer, 0)

    turn = OWN - HELD
    wrap = n_up - turn

    def near_steps(lo, hi, first, back_by):
        def body(i, r, r_ahead):
            if lo:
                for k in range(2):
                    fetched(2 * r + k, 2 * d)
            later = 2 * i + 4
            tile = later + turn - jnp.where(later >= n_up, n_up + turn, jnp.where(later >= wrap, n_up, 0))
            for k in range(2):

                @pl.when((i >= 1) & (later + k <= n_up + 2))
                def _():
                    fetch_up(tile + k, 2 * r_ahead + k)

            with jax.named_scope("near_up"):
                up(first, n_near, 2 * i + turn - back_by, 2 * r, 2)

        thirds(lo, hi, body)

    def later_steps(lo, hi):
        def body(i):
            half = lax.rem(i, 2)
            for k in range(3):
                fetched(3 * half + k, 2 * d)

            @pl.when(3 * i + 3 < n_up)
            def _():
                for k in range(3):
                    fetch_up(3 * i + 3 + k, 3 - 3 * half + k)

            @pl.when(3 * i + 3 >= n_up)
            def _():
                fetch_down(0, 0)

            with jax.named_scope("up"):
                up(lo, hi, 3 * i, 3 * half, 3)

        loop(0, n_up // 3, body)

    def down_steps(lo, hi, body, after=None, held=1):
        def step(i, r, r_ahead):
            fetched(2 * r, ff)
            if held == 1:

                @pl.when(i == 0)
                def _():
                    fetch_down(1, 1)

            @pl.when(i + 2 < n_down)
            def _():
                fetch_down(i + 2, r_ahead)

            if after:
                for k in range(2):

                    @pl.when(i == n_down - 2 + k)
                    def _():
                        after(k)

            with jax.named_scope("down"):
                body(i, r)

        thirds(lo, hi, step)

    def fetch_three_up(k):
        if k == 0:
            fetch_up(0, 0)
            fetch_up(1, 1)
        else:
            fetch_up(2, 2)

    def result(p, c, n, send_sem, recv_sem):
        cols = pl.ds(pl.multiple_of(c * COLS, COLS), n * COLS)
        return pltpu.make_async_remote_copy(
            src_ref=z.at[rows(p, p + 1), cols],
            dst_ref=back.at[rows(mirror[p], mirror[p] + 1), cols],
            send_sem=send_sem,
            recv_sem=recv_sem,
            device_id=device(p),
            device_id_type=MESH,
        )

    def send_results(lo, hi, c, n, piece, send_sem, recv_sem):
        for p in range(lo, hi):
            result(p, c, n, send_sem, recv_sem.at[piece]).start()

    def results_arrived(lo, hi, c, n, piece, recv_sem, name):
        got = back.at[rows(lo, hi), pl.ds(pl.multiple_of(c * COLS, COLS), n * COLS)]
        with jax.named_scope(name):
            pltpu.make_async_copy(got, got, recv_sem.at[piece]).wait()

    def down(lo, hi):
        at = rows(lo, hi)

        def body(i, s):
            out = jnp.dot(h[at, :], w[pl.ds(pl.multiple_of(4 * s * d, COLS), ff), :], preferred_element_type=F32)
            z[at, pl.ds(pl.multiple_of(i * COLS, COLS), COLS)] = out.astype(BF16)

        return body

    def down_near(i, s):
        cols = pl.ds(pl.multiple_of(i * COLS, COLS), COLS)
        out = jnp.dot(h[rows(0, n_near), :], w[pl.ds(pl.multiple_of(4 * s * d, COLS), ff), :], preferred_element_type=F32).astype(BF16)
        back[rows(0, 1), cols] = out[:slots]
        z[rows(1, n_near), cols] = out[slots:]

    def write(c):
        cols = pl.ds(pl.multiple_of(c * COLS, COLS), COLS)
        return pltpu.make_async_copy(back.at[pl.ds(0, tokens), cols], y_ref.at[:, cols], y_sem)

    def add_up(c):
        cols = pl.ds(pl.multiple_of(c * COLS, COLS), COLS)
        total = jnp.dot(comb[...], back[:, cols], preferred_element_type=F32)
        back[pl.ds(0, tokens), cols] = total.astype(BF16)

    def near_and_add(i, s):
        add_up(i - LAG)
        down_near(i, s)
        write(i - LAG).start()

    loop(0, OWN, own_step)
    arrived(1, n_near)
    for p in range(n_end, members):
        send(p).start()
    near_steps(0, HELD // 2, 1, 0)
    near_steps(HELD // 2, wrap // 2, 0, 0)
    near_steps(wrap // 2, n_up // 2, 1, n_up)
    arrived(n_end, members)
    for p in range(n_near, n_end):
        send(p).start()
    for p in range(n_end, members):
        with jax.named_scope("sent_rest"):
            send(p).wait_send()
    later_steps(n_end, members)
    down_steps(0, n_down, down(n_end, members), fetch_three_up)
    for p in range(n_end, members):
        result(p, 0, n_down, far_s, far_r).start()
    arrived(n_near, n_end)
    with jax.named_scope("sent_mid"):
        for p in range(1, n_end):
            send(p).wait_send()
    later_steps(n_near, n_end)

    def mid_part(q, carry):
        down_steps(3 * q, 3 * q + 3, down(n_near, n_end), lambda k: fetch_down(k, k))
        send_results(n_near, n_end, 3 * q, 3, q, mid_s, mid_r)
        return carry

    lax.fori_loop(0, n_down // 3, mid_part, 0)

    parts = n_down // 3 - 1

    def near_part(q, carry):
        down_steps(3 * q, 3 * q + 3, down_near, held=2)
        send_results(1, n_near, 3 * q, 3, q, near_s, near_r)
        return carry

    def part_arrived(q):
        results_arrived(n_near, n_end, 3 * q, 3, q, mid_r, "mid")
        results_arrived(1, n_near, 3 * q, 3, q, near_r, "near")

    def near_part_and_add(q, carry):
        part_arrived(q - LAG // 3)
        down_steps(3 * q, 3 * q + 3, near_and_add, held=2)
        send_results(1, n_near, 3 * q, 3, q, near_s, near_r)
        return carry

    lax.fori_loop(0, LAG // 3, near_part, 0)
    got = back.at[rows(n_end, members)]
    with jax.named_scope("far"):
        pltpu.make_async_copy(got, got, far_r).wait()
    lax.fori_loop(LAG // 3, parts, near_part_and_add, 0)
    part_arrived(parts - LAG // 3)

    def last(i, s):
        near_and_add(i, s)
        send_results(1, n_near, i, 1, i - 2 * parts, near_s, near_r)

    down_steps(3 * parts, n_down, last, held=2)
    for q in range(parts + 1 - LAG // 3, parts):
        part_arrived(q)
        for c in range(3 * q, 3 * q + 3):
            add_up(c)
        for c in range(3 * q, 3 * q + 3):
            write(c).start()
    results_arrived(n_near, n_end, 3 * parts, 3, parts, mid_r, "mid")
    for c in range(3 * parts, n_down):
        results_arrived(1, n_near, c, 1, c - 2 * parts, near_r, "near")
        add_up(c)
        write(c).start()
    with jax.named_scope("written"):
        for c in range(n_down):
            write(c).wait()
    gone = z.at[rows(n_end, members)]
    pltpu.make_async_copy(gone, gone, far_s).wait()
    gone = z.at[rows(n_near, n_end)]
    pltpu.make_async_copy(gone, gone, mid_s).wait()
    gone = z.at[rows(1, n_near)]
    pltpu.make_async_copy(gone, gone, near_s).wait()


def solution(mesh):
    members = mesh.shape["ep"]
    side = math.isqrt(members)

    def layer(x, expert, slot, gate, w_gate, w_up, w_down):
        tokens, d = x.shape[2:]
        ff, top = w_gate.shape[2], expert.shape[3]
        slots = 5 * tokens * top // (4 * members)
        total = members * slots
        any_ = pl.BlockSpec(memory_space=pl.ANY)
        vmem = pl.BlockSpec(memory_space=pltpu.VMEM)
        turned = lambda v: v.reshape(tokens, top).T
        y = pl.pallas_call(
            functools.partial(kernel, side, slots),
            out_shape=jax.ShapeDtypeStruct((tokens, d), BF16),
            in_specs=[any_, vmem, vmem, vmem, any_, any_, any_],
            out_specs=any_,
            scratch_shapes=[
                pltpu.VMEM((total, d), BF16),
                pltpu.VMEM((total, ff), BF16),
                pltpu.VMEM((total, d), BF16),
                pltpu.VMEM((2 * HELD * d, COLS), BF16),
                pltpu.VMEM((tokens, total), BF16),
                pltpu.SemaphoreType.DMA,
                pltpu.SemaphoreType.DMA((HELD,)),
                pltpu.SemaphoreType.DMA,
                pltpu.SemaphoreType.DMA((members,)),
                pltpu.SemaphoreType.DMA((members,)),
                pltpu.SemaphoreType.DMA,
                pltpu.SemaphoreType.DMA,
                pltpu.SemaphoreType.DMA,
                pltpu.SemaphoreType.DMA((d // COLS,)),
                pltpu.SemaphoreType.DMA,
                pltpu.SemaphoreType.DMA((d // COLS,)),
            ],
            compiler_params=pltpu.CompilerParams(
                collective_id=0, has_side_effects=True, vmem_limit_bytes=67_043_328
            ),
            name="moe",
        )(
            x.reshape(tokens, d), turned(expert), turned(slot), turned(gate),
            w_gate.reshape(d, ff), w_up.reshape(d, ff), w_down.reshape(ff, d),
        )
        return y.reshape(1, 1, tokens, d)

    per_device, per_expert = P("dp", "ep", None, None), P("ep", None, None)
    return jax.shard_map(
        layer,
        mesh=mesh,
        in_specs=(per_device,) * 4 + (per_expert,) * 3,
        out_specs=per_device,
        check_vma=False,
    )
```

```python
import functools
import math

import jax
import jax.numpy as jnp
from jax import lax
from jax.experimental import pallas as pl
from jax.experimental.pallas import tpu as pltpu
from jax.sharding import PartitionSpec as P

MESH = pl.DeviceIdType.MESH
F32, BF16 = jnp.float32, jnp.bfloat16
COLS = 256
HELD = 6
OWN = 12
LAG = 2


def plan(side):
    far = lambda v: min(v, side - v)
    peers = sorted(((far(a) + far(b), a, b) for a in range(side) for b in range(side)))
    near = [(a, b) for n, a, b in peers if n <= 1]
    mid = [(a, b) for n, a, b in peers if n == 2]
    mid.sort(key=lambda o: (2 * o[0] == side, o[0], o[1] if o[0] == 1 else -o[1]))
    rest = [(a, b) for n, a, b in peers if n > 2]
    rest.sort(key=lambda o: (-far(o[0]) - far(o[1]), -far(o[0])))
    return near, mid, rest


def kernel(
    side, slots, x_ref, expert_ref, slot_ref, gate_ref, wg_ref, wu_ref, wd_ref, y_ref,
    z, h, back, kept, w, comb, x_sem, w_sem, y_sem, out_s, out_r, far_s, far_r, mid_s, mid_r, near_s, near_r,
):
    tokens, d = x_ref.shape
    ff = wd_ref.shape[0]
    near, mid, rest = plan(side)
    order = near + mid + rest
    where = {o: p for p, o in enumerate(order)}
    mirror = [where[(-a) % side, (-b) % side] for a, b in order]
    members = len(order)
    n_near, n_end = len(near), len(near) + len(mid)
    rows = lambda lo, hi: pl.ds(lo * slots, (hi - lo) * slots)
    me = lax.axis_index("ep")
    my_x, my_y = me // side, lax.rem(me, side)

    def device(p):
        a, b = order[p]
        return {"ep": lax.rem(my_x + a, side) * side + lax.rem(my_y + b, side)}

    x_at = h.at[pl.ds(n_near * slots, tokens), pl.ds(d, d)]
    x_copy = pltpu.make_async_copy(x_ref, x_at, x_sem)
    x_copy.start()

    barrier = pltpu.get_barrier_semaphore()
    for p in range(1, members):
        pl.semaphore_signal(barrier, inc=1, device_id=device(p), device_id_type=MESH)

    def hidden(lo, hi):
        down_by = n_end - n_near if lo >= n_end else 0
        return rows(lo - down_by, hi - down_by)

    def staged(p):
        if p < n_near:
            return h.at[rows(n_near + p - 1, n_near + p), pl.ds(2 * d, d)]
        if p < n_end:
            return kept.at[rows(p - n_near, p - n_near + 1)]
        return h.at[hidden(p, p + 1), pl.ds(0, d)]

    n_up, n_down = ff // COLS, d // COLS

    def start(place, q):
        gap = 4 * ff - 2 * HELD * d
        upper = (gap if place >= HELD // 2 else 0) if isinstance(place, int) else jnp.where(place >= HELD // 2, gap, 0)
        return pl.multiple_of((2 * place + q) * d + upper, COLS)

    def fetch_up(tile, place):
        at = pl.ds(pl.multiple_of(tile * COLS, COLS), COLS)
        for q, ref in enumerate((wg_ref, wu_ref)):
            pltpu.make_async_copy(ref.at[:, at], w.at[pl.ds(start(place, q), d)], w_sem.at[place]).start()

    def fetch_down(pair, place):
        for q in range(2):
            at = pl.ds(pl.multiple_of((2 * pair + q) * COLS, COLS), COLS)
            pltpu.make_async_copy(wd_ref.at[:, at], w.at[down_rows(place, q)], w_sem.at[HELD + place]).start()

    def down_rows(place, q):
        return pl.ds(pl.multiple_of((2 * place + q) * ff, COLS), ff)

    def wait_for(got, sem):
        with jax.named_scope("weights"):
            pltpu.make_async_copy(got, got, sem).wait()

    def fetched(place):
        wait_for(w.at[pl.ds(start(place, 0), 2 * d)], w_sem.at[place])

    def loop(lo, hi, body):
        def step(i, carry):
            body(i)
            return carry

        lax.fori_loop(lo, hi, step, 0)

    expert, slot = expert_ref[...], slot_ref[...]
    off = lax.rem(expert // side - my_x + side, side) * side + lax.rem(lax.rem(expert, side) - my_y + side, side)
    place = jnp.zeros_like(off)
    for p, (a, b) in enumerate(order):
        place = jnp.where(off == a * side + b, p, place)
    code = jnp.where(slot < slots, place * slots + slot, -1)
    gate = gate_ref[...].astype(BF16).astype(F32)

    def chosen(lo, n, value):
        row = lax.broadcasted_iota(jnp.int32, (n, tokens), 0) + lo
        out = jnp.zeros((n, tokens), F32)
        for j in range(code.shape[0]):
            out = jnp.where(row == code[j : j + 1, :], value(j), out)
        return out

    def picked(lo, hi):
        return chosen(lo * slots, (hi - lo) * slots, lambda j: 1.0).astype(BF16)

    def block_rows(lo, hi, pick, at, half=None):
        first, end = (0, d) if half is None else (half * d // 2, (half + 1) * d // 2)
        for c in range(first, end, 2 * COLS):
            cols = pl.ds(c, min(2 * COLS, end - c))
            got = jnp.dot(pick, x_at[:, cols], preferred_element_type=F32).astype(BF16)
            for p in range(lo, hi):
                at(p)[:, cols] = got[(p - lo) * slots : (p - lo + 1) * slots]

    def send(p, half=None):
        cols = pl.ds(0, d) if half is None else pl.ds(half * d // 2, d // 2)
        return pltpu.make_async_remote_copy(
            src_ref=staged(p).at[:, cols],
            dst_ref=z.at[rows(mirror[p], mirror[p] + 1), cols],
            send_sem=out_s.at[p],
            recv_sem=out_r.at[mirror[p]],
            device_id=device(p),
            device_id_type=MESH,
        )

    def arrived(lo, hi):
        for p in range(lo, hi):
            got = z.at[rows(p, p + 1)]
            with jax.named_scope(f"arrive{p}"):
                pltpu.make_async_copy(got, got, out_r.at[p]).wait()

    with jax.named_scope("x"):
        x_copy.wait()
    for i in range(HELD - 1):
        fetch_up(i, i)
    pick = picked(1, n_near)
    block_rows(1, n_near, pick, staged, 0)
    with jax.named_scope("barrier"):
        pl.semaphore_wait(barrier, members - 1)
    for p in range(1, n_near):
        send(p, 0).start()
    block_rows(1, n_near, pick, staged, 1)
    for p in range(1, n_near):
        send(p, 1).start()
    with jax.named_scope("rows"):
        block_rows(n_end, members, picked(n_end, members), staged)
        block_rows(n_near, n_end, picked(n_near, n_end), staged)
        block_rows(0, 1, picked(0, 1), lambda p: z.at[rows(0, 1)])
    for c in range(0, members * slots, 128):
        part = chosen(c, 128, lambda j: gate[j : j + 1, :])
        comb[:, pl.ds(c, 128)] = part.T.astype(BF16)

    def up(lo, hi, tile, place, n):
        for k in range(n):
            g, u = (
                jnp.dot(z[rows(lo, hi), :], w[pl.ds(start(place + k, q), d), :], preferred_element_type=F32)
                for q in range(2)
            )
            cols = pl.ds(pl.multiple_of((tile + k) * COLS, COLS), COLS)
            h[hidden(lo, hi), cols] = (jax.nn.silu(g) * u).astype(BF16)

    def own_step(j):
        place = j - jnp.where(j >= HELD, HELD, 0)
        fetched(place)
        later = j + HELD - 1

        @pl.when(later < OWN)
        def _():
            fetch_up(later, later - jnp.where(later >= HELD, HELD, 0))

        with jax.named_scope("own"):
            up(0, 1, j, place, 1)

    def thirds(lo, hi, body):
        def outer(o, carry):
            loop(0, 3, lambda r: body(3 * o + r, r, jnp.where(r == 0, 2, r - 1)))
            return carry

        lax.fori_loop(lo // 3, hi // 3, outer, 0)

    turn = OWN - HELD
    wrap = n_up - turn

    def near_steps(lo, hi, first, back_by):
        def body(i, r, r_ahead):
            if lo:
                for k in range(2):
                    fetched(2 * r + k)
            later = 2 * i + 4
            tile = later + turn - jnp.where(later >= n_up, n_up + turn, jnp.where(later >= wrap, n_up, 0))
            for k in range(2):

                @pl.when((i >= 1) & (later + k <= n_up + 2))
                def _():
                    fetch_up(tile + k, 2 * r_ahead + k)

            with jax.named_scope("near_up"):
                up(first, n_near, 2 * i + turn - back_by, 2 * r, 2)

        thirds(lo, hi, body)

    def later_steps(lo, hi):
        def body(i):
            half = lax.rem(i, 2)
            for k in range(3):
                fetched(3 * half + k)

            @pl.when(3 * i + 3 < n_up)
            def _():
                for k in range(3):
                    fetch_up(3 * i + 3 + k, 3 - 3 * half + k)

            @pl.when(3 * i + 3 >= n_up)
            def _():
                fetch_down(0, 0)

            with jax.named_scope("up"):
                up(lo, hi, 3 * i, 3 * half, 3)

        loop(0, n_up // 3, body)

    def fetch_three_up():
        for k in range(HELD // 2):
            fetch_up(k, k)

    n_pairs = n_down // 2

    def down_steps(lo, hi, body, after=None):
        def step(i):
            place = lax.rem(i, 2)
            wait_for(w.at[pl.ds(pl.multiple_of(2 * place * ff, COLS), 2 * ff)], w_sem.at[HELD + place])

            @pl.when(i + 1 < n_pairs)
            def _():
                fetch_down(i + 1, 1 - place)

            if after:
                pl.when(i + 1 == n_pairs)(after)
            with jax.named_scope("down"):
                body(i, place)

        loop(lo, hi, step)

    def result(p, c, n, send_sem, recv_sem):
        cols = pl.ds(pl.multiple_of(c * COLS, COLS), n * COLS)
        return pltpu.make_async_remote_copy(
            src_ref=z.at[rows(p, p + 1), cols],
            dst_ref=back.at[rows(mirror[p], mirror[p] + 1), cols],
            send_sem=send_sem,
            recv_sem=recv_sem,
            device_id=device(p),
            device_id_type=MESH,
        )

    def send_results(lo, hi, c, n, piece, send_sem, recv_sem):
        for p in range(lo, hi):
            result(p, c, n, send_sem, recv_sem.at[piece]).start()

    def results_arrived(lo, hi, c, n, piece, recv_sem, name):
        got = back.at[rows(lo, hi), pl.ds(pl.multiple_of(c * COLS, COLS), n * COLS)]
        with jax.named_scope(name):
            pltpu.make_async_copy(got, got, recv_sem.at[piece]).wait()

    def chunk(c):
        return pl.ds(pl.multiple_of(c * COLS, COLS), COLS)

    def product(lo, hi, place, q):
        lhs = h[hidden(lo, hi), :]
        return jnp.dot(lhs, w[down_rows(place, q), :], preferred_element_type=F32).astype(BF16)

    def down(lo, hi):
        def body(i, place):
            for q in range(2):
                z[rows(lo, hi), chunk(2 * i + q)] = product(lo, hi, place, q)

        return body

    def down_near(i, place):
        for q in range(2):
            out = product(0, n_near, place, q)
            back[rows(0, 1), chunk(2 * i + q)] = out[:slots]
            z[rows(1, n_near), chunk(2 * i + q)] = out[slots:]

    def write(c, n):
        cols = pl.ds(pl.multiple_of(c * COLS, COLS), n * COLS)
        return pltpu.make_async_copy(back.at[pl.ds(0, tokens), cols], y_ref.at[:, cols], y_sem)

    def add_up(c, n):
        cols = pl.ds(pl.multiple_of(c * COLS, COLS), n * COLS)
        total = jnp.dot(comb[...], back[:, cols], preferred_element_type=F32)
        back[pl.ds(0, tokens), cols] = total.astype(BF16)

    def near_and_add(i, place):
        add_up(2 * (i - LAG), 2)
        down_near(i, place)
        write(2 * (i - LAG), 2).start()

    loop(0, OWN, own_step)
    arrived(1, n_near)
    for p in range(n_end, members):
        send(p).start()
    near_steps(0, HELD // 2, 1, 0)
    near_steps(HELD // 2, wrap // 2, 0, 0)
    near_steps(wrap // 2, n_up // 2, 1, n_up)
    arrived(n_end, members)
    for p in range(n_near, n_end):
        send(p).start()
    with jax.named_scope("sent_near_rest"):
        for p in [*range(1, n_near), *range(n_end, members)]:
            send(p).wait_send()
    later_steps(n_end, members)
    down_steps(0, n_pairs, down(n_end, members), fetch_three_up)
    for p in range(n_end, members):
        result(p, 0, n_down, far_s, far_r).start()
    arrived(n_near, n_end)
    with jax.named_scope("sent_mid"):
        for p in range(n_near, n_end):
            send(p).wait_send()
    later_steps(n_near, n_end)

    def mid_step(i, place):
        down(n_near, n_end)(i, place)
        send_results(n_near, n_end, 2 * i, 2, i, mid_s, mid_r)

    down_steps(0, n_pairs, mid_step, lambda: fetch_down(0, 0))

    def send_near(i):
        send_results(1, n_near, 2 * i, 2, i, near_s, near_r)

    def near_step(i, place):
        down_near(i, place)
        send_near(i)

    def arrived_back(i):
        results_arrived(n_near, n_end, 2 * i, 2, i, mid_r, "mid")
        results_arrived(1, n_near, 2 * i, 2, i, near_r, "near")

    def near_step_and_add(i, place):
        arrived_back(i - LAG)
        near_and_add(i, place)
        send_near(i)

    def last_step(i, place):
        def one(q):
            z[rows(1, n_near), chunk(2 * i + q)] = product(1, n_near, place, q)
            send_results(1, n_near, 2 * i + q, 1, n_pairs - 1 + q, near_s, near_r)

        loop(0, 2, one)
        for q in range(2):
            back[rows(0, 1), chunk(2 * i + q)] = product(0, 1, place, q)

    down_steps(0, LAG, near_step)
    got = back.at[rows(n_end, members)]
    with jax.named_scope("far"):
        pltpu.make_async_copy(got, got, far_r).wait()
    down_steps(LAG, n_pairs - 1, near_step_and_add)
    down_steps(n_pairs - 1, n_pairs, last_step)
    for i in range(n_pairs - 1 - LAG, n_pairs - 1):
        arrived_back(i)
        add_up(2 * i, 2)
        write(2 * i, 2).start()
    results_arrived(n_near, n_end, n_down - 2, 2, n_pairs - 1, mid_r, "mid")
    for q in range(2):
        results_arrived(1, n_near, n_down - 2 + q, 1, n_pairs - 1 + q, near_r, "near")
        add_up(n_down - 2 + q, 1)
        write(n_down - 2 + q, 1).start()
    with jax.named_scope("written"):
        for i in range(n_pairs - 1):
            write(2 * i, 2).wait()
        for q in range(2):
            write(n_down - 2 + q, 1).wait()
    gone = z.at[rows(n_end, members)]
    pltpu.make_async_copy(gone, gone, far_s).wait()
    gone = z.at[rows(n_near, n_end)]
    pltpu.make_async_copy(gone, gone, mid_s).wait()
    gone = z.at[rows(1, n_near)]
    pltpu.make_async_copy(gone, gone, near_s).wait()


def solution(mesh):
    members = mesh.shape["ep"]
    side = math.isqrt(members)

    def layer(x, expert, slot, gate, w_gate, w_up, w_down):
        tokens, d = x.shape[2:]
        ff, top = w_gate.shape[2], expert.shape[3]
        slots = 5 * tokens * top // (4 * members)
        total = members * slots
        n_near, n_mid, n_rest = map(len, plan(side))
        any_ = pl.BlockSpec(memory_space=pl.ANY)
        vmem = pl.BlockSpec(memory_space=pltpu.VMEM)
        turned = lambda v: v.reshape(tokens, top).T
        y = pl.pallas_call(
            functools.partial(kernel, side, slots),
            out_shape=jax.ShapeDtypeStruct((tokens, d), BF16),
            in_specs=[any_, vmem, vmem, vmem, any_, any_, any_],
            out_specs=any_,
            scratch_shapes=[
                pltpu.VMEM((total, d), BF16),
                pltpu.VMEM(((n_near + max(n_mid, n_rest)) * slots, ff), BF16),
                pltpu.VMEM((total, d), BF16),
                pltpu.VMEM((n_mid * slots, d), BF16),
                pltpu.VMEM((4 * ff, COLS), BF16),
                pltpu.VMEM((tokens, total), BF16),
                pltpu.SemaphoreType.DMA,
                pltpu.SemaphoreType.DMA((HELD + 2,)),
                pltpu.SemaphoreType.DMA,
                pltpu.SemaphoreType.DMA((members,)),
                pltpu.SemaphoreType.DMA((members,)),
                pltpu.SemaphoreType.DMA,
                pltpu.SemaphoreType.DMA,
                pltpu.SemaphoreType.DMA,
                pltpu.SemaphoreType.DMA((d // COLS,)),
                pltpu.SemaphoreType.DMA,
                pltpu.SemaphoreType.DMA((d // COLS,)),
            ],
            compiler_params=pltpu.CompilerParams(
                collective_id=0, has_side_effects=True, vmem_limit_bytes=67_043_328
            ),
            name="moe",
        )(
            x.reshape(tokens, d), turned(expert), turned(slot), turned(gate),
            w_gate.reshape(d, ff), w_up.reshape(d, ff), w_down.reshape(ff, d),
        )
        return y.reshape(1, 1, tokens, d)

    per_device, per_expert = P("dp", "ep", None, None), P("ep", None, None)
    return jax.shard_map(
        layer,
        mesh=mesh,
        in_specs=(per_device,) * 4 + (per_expert,) * 3,
        out_specs=per_device,
        check_vma=False,
    )
```

```python
import functools
import math

import jax
import jax.numpy as jnp
from jax import lax
from jax.experimental import pallas as pl
from jax.experimental.pallas import tpu as pltpu
from jax.sharding import PartitionSpec as P

MESH = pl.DeviceIdType.MESH
F32, BF16 = jnp.float32, jnp.bfloat16
COLS = 256
HELD = 6
OWN = 12
LAG = 3


def plan(side):
    far = lambda v: min(v, side - v)
    peers = sorted(((far(a) + far(b), a, b) for a in range(side) for b in range(side)))
    near = [(a, b) for n, a, b in peers if n <= 1]
    mid = [(a, b) for n, a, b in peers if n == 2]
    mid.sort(key=lambda o: (2 * o[0] == side, o[0], o[1] if o[0] == 1 else -o[1]))
    rest = [(a, b) for n, a, b in peers if n > 2]
    rest.sort(key=lambda o: (-far(o[0]) - far(o[1]), -far(o[0])))
    return near, mid, rest


def kernel(
    side, slots, x_ref, expert_ref, slot_ref, gate_ref, wg_ref, wu_ref, wd_ref, y_ref,
    z, h, back, kept, w, comb, x_sem, w_sem, y_sem, out_s, out_r, far_s, far_r, mid_s, mid_r, near_s, near_r,
):
    tokens, d = x_ref.shape
    ff = wd_ref.shape[0]
    near, mid, rest = plan(side)
    order = near + mid + rest
    where = {o: p for p, o in enumerate(order)}
    mirror = [where[(-a) % side, (-b) % side] for a, b in order]
    members = len(order)
    n_near, n_end = len(near), len(near) + len(mid)
    rows = lambda lo, hi: pl.ds(lo * slots, (hi - lo) * slots)
    me = lax.axis_index("ep")
    my_x, my_y = me // side, lax.rem(me, side)

    def device(p):
        a, b = order[p]
        return {"ep": lax.rem(my_x + a, side) * side + lax.rem(my_y + b, side)}

    x_at = h.at[pl.ds(n_near * slots, tokens), pl.ds(d, d)]
    x_copy = pltpu.make_async_copy(x_ref, x_at, x_sem)
    x_copy.start()

    barrier = pltpu.get_barrier_semaphore()
    for p in range(1, members):
        pl.semaphore_signal(barrier, inc=1, device_id=device(p), device_id_type=MESH)

    def hidden(lo, hi):
        down_by = n_end - n_near if lo >= n_end else 0
        return rows(lo - down_by, hi - down_by)

    def staged(p):
        if p < n_near:
            return h.at[rows(n_near + p - 1, n_near + p), pl.ds(2 * d, d)]
        if p < n_end:
            return kept.at[rows(p - n_near, p - n_near + 1)]
        return h.at[hidden(p, p + 1), pl.ds(0, d)]

    n_up, n_down = ff // COLS, d // COLS

    def start(place, q):
        gap = 4 * ff - 2 * HELD * d
        upper = (gap if place >= HELD // 2 else 0) if isinstance(place, int) else jnp.where(place >= HELD // 2, gap, 0)
        return pl.multiple_of((2 * place + q) * d + upper, COLS)

    def fetch_up(tile, place):
        at = pl.ds(pl.multiple_of(tile * COLS, COLS), COLS)
        for q, ref in enumerate((wg_ref, wu_ref)):
            pltpu.make_async_copy(ref.at[:, at], w.at[pl.ds(start(place, q), d)], w_sem.at[place]).start()

    def fetch_down(pair, place):
        for q in range(2):
            at = pl.ds(pl.multiple_of((2 * pair + q) * COLS, COLS), COLS)
            pltpu.make_async_copy(wd_ref.at[:, at], w.at[down_rows(place, q)], w_sem.at[HELD + place]).start()

    def down_rows(place, q):
        return pl.ds(pl.multiple_of((2 * place + q) * ff, COLS), ff)

    def wait_for(got, sem):
        with jax.named_scope("weights"):
            pltpu.make_async_copy(got, got, sem).wait()

    def fetched(place):
        wait_for(w.at[pl.ds(start(place, 0), 2 * d)], w_sem.at[place])

    def loop(lo, hi, body):
        def step(i, carry):
            body(i)
            return carry

        lax.fori_loop(lo, hi, step, 0)

    expert, slot = expert_ref[...], slot_ref[...]
    off = lax.rem(expert // side - my_x + side, side) * side + lax.rem(lax.rem(expert, side) - my_y + side, side)
    place = jnp.zeros_like(off)
    for p, (a, b) in enumerate(order):
        place = jnp.where(off == a * side + b, p, place)
    code = jnp.where(slot < slots, place * slots + slot, -1)
    gate = gate_ref[...].astype(BF16).astype(F32)

    def chosen(lo, n, value):
        row = lax.broadcasted_iota(jnp.int32, (n, tokens), 0) + lo
        out = jnp.zeros((n, tokens), F32)
        for j in range(code.shape[0]):
            out = jnp.where(row == code[j : j + 1, :], value(j), out)
        return out

    def picked(lo, hi):
        return chosen(lo * slots, (hi - lo) * slots, lambda j: 1.0).astype(BF16)

    def block_rows(lo, hi, pick, at, half=None):
        first, end = (0, d) if half is None else (half * d // 2, (half + 1) * d // 2)
        for c in range(first, end, 2 * COLS):
            cols = pl.ds(c, min(2 * COLS, end - c))
            got = jnp.dot(pick, x_at[:, cols], preferred_element_type=F32).astype(BF16)
            for p in range(lo, hi):
                at(p)[:, cols] = got[(p - lo) * slots : (p - lo + 1) * slots]

    def send(p, half=None):
        cols = pl.ds(0, d) if half is None else pl.ds(half * d // 2, d // 2)
        return pltpu.make_async_remote_copy(
            src_ref=staged(p).at[:, cols],
            dst_ref=z.at[rows(mirror[p], mirror[p] + 1), cols],
            send_sem=out_s.at[p],
            recv_sem=out_r.at[mirror[p]],
            device_id=device(p),
            device_id_type=MESH,
        )

    def arrived(lo, hi):
        for p in range(lo, hi):
            got = z.at[rows(p, p + 1)]
            with jax.named_scope(f"arrive{p}"):
                pltpu.make_async_copy(got, got, out_r.at[p]).wait()

    with jax.named_scope("x"):
        x_copy.wait()
    for i in range(HELD - 1):
        fetch_up(i, i)
    pick = picked(1, n_near)
    block_rows(1, n_near, pick, staged, 0)
    with jax.named_scope("barrier"):
        pl.semaphore_wait(barrier, members - 1)
    for p in range(1, n_near):
        send(p, 0).start()
    block_rows(1, n_near, pick, staged, 1)
    for p in range(1, n_near):
        send(p, 1).start()
    with jax.named_scope("rows"):
        block_rows(n_end, members, picked(n_end, members), staged)
        block_rows(n_near, n_end, picked(n_near, n_end), staged)
        block_rows(0, 1, picked(0, 1), lambda p: z.at[rows(0, 1)])
    for c in range(0, members * slots, 128):
        part = chosen(c, 128, lambda j: gate[j : j + 1, :])
        comb[:, pl.ds(c, 128)] = part.T.astype(BF16)

    def up(lo, hi, tile, place, n):
        for k in range(n):
            g, u = (
                jnp.dot(z[rows(lo, hi), :], w[pl.ds(start(place + k, q), d), :], preferred_element_type=F32)
                for q in range(2)
            )
            cols = pl.ds(pl.multiple_of((tile + k) * COLS, COLS), COLS)
            h[hidden(lo, hi), cols] = (jax.nn.silu(g) * u).astype(BF16)

    def own_step(j):
        place = j - jnp.where(j >= HELD, HELD, 0)
        fetched(place)
        later = j + HELD - 1

        @pl.when(later < OWN)
        def _():
            fetch_up(later, later - jnp.where(later >= HELD, HELD, 0))

        with jax.named_scope("own"):
            up(0, 1, j, place, 1)

    def thirds(lo, hi, body):
        def outer(o, carry):
            loop(0, 3, lambda r: body(3 * o + r, r, jnp.where(r == 0, 2, r - 1)))
            return carry

        lax.fori_loop(lo // 3, hi // 3, outer, 0)

    turn = OWN - HELD
    wrap = n_up - turn

    def near_steps(lo, hi, first, back_by):
        def body(i, r, r_ahead):
            if lo:
                for k in range(2):
                    fetched(2 * r + k)
            later = 2 * i + 4
            tile = later + turn - jnp.where(later >= n_up, n_up + turn, jnp.where(later >= wrap, n_up, 0))
            for k in range(2):

                @pl.when((i >= 1) & (later + k <= n_up + 2))
                def _():
                    fetch_up(tile + k, 2 * r_ahead + k)

            with jax.named_scope("near_up"):
                up(first, n_near, 2 * i + turn - back_by, 2 * r, 2)

        thirds(lo, hi, body)

    def later_steps(lo, hi):
        def body(i):
            half = lax.rem(i, 2)
            for k in range(3):
                fetched(3 * half + k)

            @pl.when(3 * i + 3 < n_up)
            def _():
                for k in range(3):
                    fetch_up(3 * i + 3 + k, 3 - 3 * half + k)

            @pl.when(3 * i + 3 >= n_up)
            def _():
                fetch_down(0, 0)

            with jax.named_scope("up"):
                up(lo, hi, 3 * i, 3 * half, 3)

        loop(0, n_up // 3, body)

    def fetch_three_up():
        for k in range(HELD // 2):
            fetch_up(k, k)

    n_pairs = n_down // 2

    def down_steps(lo, hi, body, after=None):
        def step(i):
            place = lax.rem(i, 2)
            wait_for(w.at[pl.ds(pl.multiple_of(2 * place * ff, COLS), 2 * ff)], w_sem.at[HELD + place])

            @pl.when(i + 1 < n_pairs)
            def _():
                fetch_down(i + 1, 1 - place)

            if after:
                pl.when(i + 1 == n_pairs)(after)
            with jax.named_scope("down"):
                body(i, place)

        loop(lo, hi, step)

    def result(p, c, n, send_sem, recv_sem):
        cols = pl.ds(pl.multiple_of(c * COLS, COLS), n * COLS)
        return pltpu.make_async_remote_copy(
            src_ref=z.at[rows(p, p + 1), cols],
            dst_ref=back.at[rows(mirror[p], mirror[p] + 1), cols],
            send_sem=send_sem,
            recv_sem=recv_sem,
            device_id=device(p),
            device_id_type=MESH,
        )

    def send_results(lo, hi, c, n, piece, send_sem, recv_sem):
        for p in range(lo, hi):
            result(p, c, n, send_sem, recv_sem.at[piece]).start()

    def results_arrived(lo, hi, c, n, piece, recv_sem, name):
        got = back.at[rows(lo, hi), pl.ds(pl.multiple_of(c * COLS, COLS), n * COLS)]
        with jax.named_scope(name):
            pltpu.make_async_copy(got, got, recv_sem.at[piece]).wait()

    def chunk(c):
        return pl.ds(pl.multiple_of(c * COLS, COLS), COLS)

    def product(lo, hi, place, q):
        lhs = h[hidden(lo, hi), :]
        return jnp.dot(lhs, w[down_rows(place, q), :], preferred_element_type=F32).astype(BF16)

    def down(lo, hi):
        def body(i, place):
            for q in range(2):
                z[rows(lo, hi), chunk(2 * i + q)] = product(lo, hi, place, q)

        return body

    def down_near(i, place):
        for q in range(2):
            out = product(0, n_near, place, q)
            back[rows(0, 1), chunk(2 * i + q)] = out[:slots]
            z[rows(1, n_near), chunk(2 * i + q)] = out[slots:]

    def write(c, n):
        cols = pl.ds(pl.multiple_of(c * COLS, COLS), n * COLS)
        return pltpu.make_async_copy(back.at[pl.ds(0, tokens), cols], y_ref.at[:, cols], y_sem)

    def add_up(c, n):
        cols = pl.ds(pl.multiple_of(c * COLS, COLS), n * COLS)
        total = jnp.dot(comb[...], back[:, cols], preferred_element_type=F32)
        back[pl.ds(0, tokens), cols] = total.astype(BF16)

    def near_and_add(i, place):
        add_up(2 * (i - LAG), 2)
        down_near(i, place)
        write(2 * (i - LAG), 2).start()

    loop(0, OWN, own_step)
    arrived(1, n_near)
    for p in range(n_end, members):
        send(p).start()
    near_steps(0, HELD // 2, 1, 0)
    near_steps(HELD // 2, wrap // 2, 0, 0)
    near_steps(wrap // 2, n_up // 2, 1, n_up)
    arrived(n_end, members)
    for p in range(n_near, n_end):
        send(p).start()
    with jax.named_scope("sent_near_rest"):
        for p in [*range(1, n_near), *range(n_end, members)]:
            send(p).wait_send()
    later_steps(n_end, members)
    down_steps(0, n_pairs, down(n_end, members), fetch_three_up)
    for p in range(n_end, members):
        result(p, 0, n_down, far_s, far_r).start()
    arrived(n_near, n_end)
    with jax.named_scope("sent_mid"):
        for p in range(n_near, n_end):
            send(p).wait_send()
    later_steps(n_near, n_end)

    def mid_step(i, place):
        down(n_near, n_end)(i, place)
        send_results(n_near, n_end, 2 * i, 2, i, mid_s, mid_r)

    down_steps(0, n_pairs, mid_step, lambda: fetch_down(0, 0))

    def send_near(i):
        send_results(1, n_near, 2 * i, 2, i, near_s, near_r)

    def near_step(i, place):
        down_near(i, place)
        send_near(i)

    def arrived_back(i):
        results_arrived(n_near, n_end, 2 * i, 2, i, mid_r, "mid")
        results_arrived(1, n_near, 2 * i, 2, i, near_r, "near")

    def near_step_and_add(i, place):
        arrived_back(i - LAG)
        near_and_add(i, place)
        send_near(i)

    def last_step(i, place):
        def one(q):
            z[rows(1, n_near), chunk(2 * i + q)] = product(1, n_near, place, q)
            send_results(1, n_near, 2 * i + q, 1, n_pairs - 1 + q, near_s, near_r)

        loop(0, 2, one)
        for q in range(2):
            back[rows(0, 1), chunk(2 * i + q)] = product(0, 1, place, q)

    down_steps(0, LAG, near_step)
    got = back.at[rows(n_end, members)]
    with jax.named_scope("far"):
        pltpu.make_async_copy(got, got, far_r).wait()
    down_steps(LAG, n_pairs - 1, near_step_and_add)
    down_steps(n_pairs - 1, n_pairs, last_step)
    for i in range(n_pairs - 1 - LAG, n_pairs - 1):
        arrived_back(i)
        add_up(2 * i, 2)
        write(2 * i, 2).start()
    results_arrived(n_near, n_end, n_down - 2, 2, n_pairs - 1, mid_r, "mid")
    for q in range(2):
        results_arrived(1, n_near, n_down - 2 + q, 1, n_pairs - 1 + q, near_r, "near")
        add_up(n_down - 2 + q, 1)
        write(n_down - 2 + q, 1).start()
    with jax.named_scope("written"):
        for i in range(n_pairs - 1):
            write(2 * i, 2).wait()
        for q in range(2):
            write(n_down - 2 + q, 1).wait()
    gone = z.at[rows(n_end, members)]
    pltpu.make_async_copy(gone, gone, far_s).wait()
    gone = z.at[rows(n_near, n_end)]
    pltpu.make_async_copy(gone, gone, mid_s).wait()
    gone = z.at[rows(1, n_near)]
    pltpu.make_async_copy(gone, gone, near_s).wait()


def solution(mesh):
    members = mesh.shape["ep"]
    side = math.isqrt(members)

    def layer(x, expert, slot, gate, w_gate, w_up, w_down):
        tokens, d = x.shape[2:]
        ff, top = w_gate.shape[2], expert.shape[3]
        slots = 5 * tokens * top // (4 * members)
        total = members * slots
        n_near, n_mid, n_rest = map(len, plan(side))
        any_ = pl.BlockSpec(memory_space=pl.ANY)
        vmem = pl.BlockSpec(memory_space=pltpu.VMEM)
        turned = lambda v: v.reshape(tokens, top).T
        y = pl.pallas_call(
            functools.partial(kernel, side, slots),
            out_shape=jax.ShapeDtypeStruct((tokens, d), BF16),
            in_specs=[any_, vmem, vmem, vmem, any_, any_, any_],
            out_specs=any_,
            scratch_shapes=[
                pltpu.VMEM((total, d), BF16),
                pltpu.VMEM(((n_near + max(n_mid, n_rest)) * slots, ff), BF16),
                pltpu.VMEM((total, d), BF16),
                pltpu.VMEM((n_mid * slots, d), BF16),
                pltpu.VMEM((4 * ff, COLS), BF16),
                pltpu.VMEM((tokens, total), BF16),
                pltpu.SemaphoreType.DMA,
                pltpu.SemaphoreType.DMA((HELD + 2,)),
                pltpu.SemaphoreType.DMA,
                pltpu.SemaphoreType.DMA((members,)),
                pltpu.SemaphoreType.DMA((members,)),
                pltpu.SemaphoreType.DMA,
                pltpu.SemaphoreType.DMA,
                pltpu.SemaphoreType.DMA,
                pltpu.SemaphoreType.DMA((d // COLS,)),
                pltpu.SemaphoreType.DMA,
                pltpu.SemaphoreType.DMA((d // COLS,)),
            ],
            compiler_params=pltpu.CompilerParams(
                collective_id=0, has_side_effects=True, vmem_limit_bytes=67_043_328
            ),
            name="moe",
        )(
            x.reshape(tokens, d), turned(expert), turned(slot), turned(gate),
            w_gate.reshape(d, ff), w_up.reshape(d, ff), w_down.reshape(ff, d),
        )
        return y.reshape(1, 1, tokens, d)

    per_device, per_expert = P("dp", "ep", None, None), P("ep", None, None)
    return jax.shard_map(
        layer,
        mesh=mesh,
        in_specs=(per_device,) * 4 + (per_expert,) * 3,
        out_specs=per_device,
        check_vma=False,
    )
```

```python
import functools
import math

import jax
import jax.numpy as jnp
from jax import lax
from jax.experimental import pallas as pl
from jax.experimental.pallas import tpu as pltpu
from jax.sharding import PartitionSpec as P

MESH = pl.DeviceIdType.MESH
F32, BF16 = jnp.float32, jnp.bfloat16
COLS = 256
HELD = 6
OWN = 12
LAG = 4


def plan(side):
    far = lambda v: min(v, side - v)
    peers = sorted(((far(a) + far(b), a, b) for a in range(side) for b in range(side)))
    near = [(a, b) for n, a, b in peers if n <= 1]
    mid = [(a, b) for n, a, b in peers if n == 2]
    mid.sort(key=lambda o: (2 * o[0] == side, o[0], o[1] if o[0] == 1 else -o[1]))
    rest = [(a, b) for n, a, b in peers if n > 2]
    rest.sort(key=lambda o: (-far(o[0]) - far(o[1]), -far(o[0])))
    return near, mid, rest


def kernel(
    side, slots, x_ref, expert_ref, slot_ref, gate_ref, wg_ref, wu_ref, wd_ref, y_ref,
    z, h, back, kept, w, comb, x_sem, w_sem, y_sem, out_s, out_r, far_s, far_r, mid_s, mid_r, near_s, near_r,
):
    tokens, d = x_ref.shape
    ff = wd_ref.shape[0]
    near, mid, rest = plan(side)
    order = near + mid + rest
    where = {o: p for p, o in enumerate(order)}
    mirror = [where[(-a) % side, (-b) % side] for a, b in order]
    members = len(order)
    n_near, n_end = len(near), len(near) + len(mid)
    rows = lambda lo, hi: pl.ds(lo * slots, (hi - lo) * slots)
    me = lax.axis_index("ep")
    my_x, my_y = me // side, lax.rem(me, side)

    def device(p):
        a, b = order[p]
        return {"ep": lax.rem(my_x + a, side) * side + lax.rem(my_y + b, side)}

    x_at = h.at[pl.ds(n_near * slots, tokens), pl.ds(d, d)]
    x_copy = pltpu.make_async_copy(x_ref, x_at, x_sem)
    x_copy.start()

    barrier = pltpu.get_barrier_semaphore()
    for p in range(1, members):
        pl.semaphore_signal(barrier, inc=1, device_id=device(p), device_id_type=MESH)

    def hidden(lo, hi):
        down_by = n_end - n_near if lo >= n_end else 0
        return rows(lo - down_by, hi - down_by)

    def staged(p):
        if p < n_near:
            return h.at[rows(n_near + p - 1, n_near + p), pl.ds(2 * d, d)]
        if p < n_end:
            return kept.at[rows(p - n_near, p - n_near + 1)]
        return h.at[hidden(p, p + 1), pl.ds(0, d)]

    n_up, n_down = ff // COLS, d // COLS

    def start(place, q):
        gap = 4 * ff - 2 * HELD * d
        upper = (gap if place >= HELD // 2 else 0) if isinstance(place, int) else jnp.where(place >= HELD // 2, gap, 0)
        return pl.multiple_of((2 * place + q) * d + upper, COLS)

    def fetch_up(tile, place):
        at = pl.ds(pl.multiple_of(tile * COLS, COLS), COLS)
        for q, ref in enumerate((wg_ref, wu_ref)):
            pltpu.make_async_copy(ref.at[:, at], w.at[pl.ds(start(place, q), d)], w_sem.at[place]).start()

    def fetch_down(pair, place):
        for q in range(2):
            at = pl.ds(pl.multiple_of((2 * pair + q) * COLS, COLS), COLS)
            pltpu.make_async_copy(wd_ref.at[:, at], w.at[down_rows(place, q)], w_sem.at[HELD + place]).start()

    def down_rows(place, q):
        return pl.ds(pl.multiple_of((2 * place + q) * ff, COLS), ff)

    def wait_for(got, sem):
        with jax.named_scope("weights"):
            pltpu.make_async_copy(got, got, sem).wait()

    def fetched(place):
        wait_for(w.at[pl.ds(start(place, 0), 2 * d)], w_sem.at[place])

    def loop(lo, hi, body):
        def step(i, carry):
            body(i)
            return carry

        lax.fori_loop(lo, hi, step, 0)

    expert, slot = expert_ref[...], slot_ref[...]
    off = lax.rem(expert // side - my_x + side, side) * side + lax.rem(lax.rem(expert, side) - my_y + side, side)
    place = jnp.zeros_like(off)
    for p, (a, b) in enumerate(order):
        place = jnp.where(off == a * side + b, p, place)
    code = jnp.where(slot < slots, place * slots + slot, -1)
    gate = gate_ref[...].astype(BF16).astype(F32)

    def chosen(lo, n, value):
        row = lax.broadcasted_iota(jnp.int32, (n, tokens), 0) + lo
        out = jnp.zeros((n, tokens), F32)
        for j in range(code.shape[0]):
            out = jnp.where(row == code[j : j + 1, :], value(j), out)
        return out

    def picked(lo, hi):
        return chosen(lo * slots, (hi - lo) * slots, lambda j: 1.0).astype(BF16)

    def block_rows(lo, hi, pick, at, half=None):
        first, end = (0, d) if half is None else (half * d // 2, (half + 1) * d // 2)
        for c in range(first, end, 2 * COLS):
            cols = pl.ds(c, min(2 * COLS, end - c))
            got = jnp.dot(pick, x_at[:, cols], preferred_element_type=F32).astype(BF16)
            for p in range(lo, hi):
                at(p)[:, cols] = got[(p - lo) * slots : (p - lo + 1) * slots]

    def send(p, half=None):
        cols = pl.ds(0, d) if half is None else pl.ds(half * d // 2, d // 2)
        return pltpu.make_async_remote_copy(
            src_ref=staged(p).at[:, cols],
            dst_ref=z.at[rows(mirror[p], mirror[p] + 1), cols],
            send_sem=out_s.at[p],
            recv_sem=out_r.at[mirror[p]],
            device_id=device(p),
            device_id_type=MESH,
        )

    def arrived(lo, hi):
        for p in range(lo, hi):
            got = z.at[rows(p, p + 1)]
            with jax.named_scope(f"arrive{p}"):
                pltpu.make_async_copy(got, got, out_r.at[p]).wait()

    with jax.named_scope("x"):
        x_copy.wait()
    for i in range(HELD - 1):
        fetch_up(i, i)
    pick = picked(1, n_near)
    block_rows(1, n_near, pick, staged, 0)
    with jax.named_scope("barrier"):
        pl.semaphore_wait(barrier, members - 1)
    for p in range(1, n_near):
        send(p, 0).start()
    block_rows(1, n_near, pick, staged, 1)
    for p in range(1, n_near):
        send(p, 1).start()
    with jax.named_scope("rows"):
        block_rows(n_end, members, picked(n_end, members), staged)
        block_rows(n_near, n_end, picked(n_near, n_end), staged)
        block_rows(0, 1, picked(0, 1), lambda p: z.at[rows(0, 1)])
    for c in range(0, members * slots, 128):
        part = chosen(c, 128, lambda j: gate[j : j + 1, :])
        comb[:, pl.ds(c, 128)] = part.T.astype(BF16)

    def up(lo, hi, tile, place, n):
        for k in range(n):
            g, u = (
                jnp.dot(z[rows(lo, hi), :], w[pl.ds(start(place + k, q), d), :], preferred_element_type=F32)
                for q in range(2)
            )
            cols = pl.ds(pl.multiple_of((tile + k) * COLS, COLS), COLS)
            h[hidden(lo, hi), cols] = (jax.nn.silu(g) * u).astype(BF16)

    def own_step(j):
        place = j - jnp.where(j >= HELD, HELD, 0)
        fetched(place)
        later = j + HELD - 1

        @pl.when(later < OWN)
        def _():
            fetch_up(later, later - jnp.where(later >= HELD, HELD, 0))

        with jax.named_scope("own"):
            up(0, 1, j, place, 1)

    def thirds(lo, hi, body):
        def outer(o, carry):
            loop(0, 3, lambda r: body(3 * o + r, r, jnp.where(r == 0, 2, r - 1)))
            return carry

        lax.fori_loop(lo // 3, hi // 3, outer, 0)

    turn = OWN - HELD
    wrap = n_up - turn

    def near_steps(lo, hi, first, back_by):
        def body(i, r, r_ahead):
            if lo:
                for k in range(2):
                    fetched(2 * r + k)
            later = 2 * i + 4
            tile = later + turn - jnp.where(later >= n_up, n_up + turn, jnp.where(later >= wrap, n_up, 0))
            for k in range(2):

                @pl.when((i >= 1) & (later + k <= n_up + 2))
                def _():
                    fetch_up(tile + k, 2 * r_ahead + k)

            with jax.named_scope("near_up"):
                up(first, n_near, 2 * i + turn - back_by, 2 * r, 2)

        thirds(lo, hi, body)

    def later_steps(lo, hi):
        def body(i):
            half = lax.rem(i, 2)
            for k in range(3):
                fetched(3 * half + k)

            @pl.when(3 * i + 3 < n_up)
            def _():
                for k in range(3):
                    fetch_up(3 * i + 3 + k, 3 - 3 * half + k)

            @pl.when(3 * i + 3 >= n_up)
            def _():
                fetch_down(0, 0)

            with jax.named_scope("up"):
                up(lo, hi, 3 * i, 3 * half, 3)

        loop(0, n_up // 3, body)

    def fetch_three_up():
        for k in range(HELD // 2):
            fetch_up(k, k)

    n_pairs = n_down // 2

    def down_steps(lo, hi, body, after=None):
        def step(i):
            place = lax.rem(i, 2)
            wait_for(w.at[pl.ds(pl.multiple_of(2 * place * ff, COLS), 2 * ff)], w_sem.at[HELD + place])

            @pl.when(i + 1 < n_pairs)
            def _():
                fetch_down(i + 1, 1 - place)

            if after:
                pl.when(i + 1 == n_pairs)(after)
            with jax.named_scope("down"):
                body(i, place)

        loop(lo, hi, step)

    def result(p, c, n, send_sem, recv_sem):
        cols = pl.ds(pl.multiple_of(c * COLS, COLS), n * COLS)
        return pltpu.make_async_remote_copy(
            src_ref=z.at[rows(p, p + 1), cols],
            dst_ref=back.at[rows(mirror[p], mirror[p] + 1), cols],
            send_sem=send_sem,
            recv_sem=recv_sem,
            device_id=device(p),
            device_id_type=MESH,
        )

    def send_results(lo, hi, c, n, piece, send_sem, recv_sem):
        for p in range(lo, hi):
            result(p, c, n, send_sem, recv_sem.at[piece]).start()

    def results_arrived(lo, hi, c, n, piece, recv_sem, name):
        got = back.at[rows(lo, hi), pl.ds(pl.multiple_of(c * COLS, COLS), n * COLS)]
        with jax.named_scope(name):
            pltpu.make_async_copy(got, got, recv_sem.at[piece]).wait()

    def chunk(c):
        return pl.ds(pl.multiple_of(c * COLS, COLS), COLS)

    def product(lo, hi, place, q):
        lhs = h[hidden(lo, hi), :]
        return jnp.dot(lhs, w[down_rows(place, q), :], preferred_element_type=F32).astype(BF16)

    def down(lo, hi):
        def body(i, place):
            for q in range(2):
                z[rows(lo, hi), chunk(2 * i + q)] = product(lo, hi, place, q)

        return body

    def down_near(i, place):
        for q in range(2):
            out = product(0, n_near, place, q)
            back[rows(0, 1), chunk(2 * i + q)] = out[:slots]
            z[rows(1, n_near), chunk(2 * i + q)] = out[slots:]

    def write(c, n):
        cols = pl.ds(pl.multiple_of(c * COLS, COLS), n * COLS)
        return pltpu.make_async_copy(back.at[pl.ds(0, tokens), cols], y_ref.at[:, cols], y_sem)

    def add_up(c, n):
        cols = pl.ds(pl.multiple_of(c * COLS, COLS), n * COLS)
        total = jnp.dot(comb[...], back[:, cols], preferred_element_type=F32)
        back[pl.ds(0, tokens), cols] = total.astype(BF16)

    def near_and_add(i, place):
        add_up(2 * (i - LAG), 2)
        down_near(i, place)
        write(2 * (i - LAG), 2).start()

    loop(0, OWN, own_step)
    arrived(1, n_near)
    for p in range(n_end, members):
        send(p).start()
    near_steps(0, HELD // 2, 1, 0)
    near_steps(HELD // 2, wrap // 2, 0, 0)
    near_steps(wrap // 2, n_up // 2, 1, n_up)
    arrived(n_end, members)
    for p in range(n_near, n_end):
        send(p).start()
    with jax.named_scope("sent_near_rest"):
        for p in [*range(1, n_near), *range(n_end, members)]:
            send(p).wait_send()
    later_steps(n_end, members)
    down_steps(0, n_pairs, down(n_end, members), fetch_three_up)
    for p in range(n_end, members):
        result(p, 0, n_down, far_s, far_r).start()
    arrived(n_near, n_end)
    with jax.named_scope("sent_mid"):
        for p in range(n_near, n_end):
            send(p).wait_send()
    later_steps(n_near, n_end)

    def mid_step(i, place):
        down(n_near, n_end)(i, place)
        send_results(n_near, n_end, 2 * i, 2, i, mid_s, mid_r)

    down_steps(0, n_pairs, mid_step, lambda: fetch_down(0, 0))

    def send_near(i):
        send_results(1, n_near, 2 * i, 2, i, near_s, near_r)

    def near_step(i, place):
        down_near(i, place)
        send_near(i)

    def arrived_back(i):
        results_arrived(n_near, n_end, 2 * i, 2, i, mid_r, "mid")
        results_arrived(1, n_near, 2 * i, 2, i, near_r, "near")

    def near_step_and_add(i, place):
        arrived_back(i - LAG)
        near_and_add(i, place)
        send_near(i)

    def last_step(i, place):
        def one(q):
            z[rows(1, n_near), chunk(2 * i + q)] = product(1, n_near, place, q)
            send_results(1, n_near, 2 * i + q, 1, n_pairs - 1 + q, near_s, near_r)

        loop(0, 2, one)
        for q in range(2):
            back[rows(0, 1), chunk(2 * i + q)] = product(0, 1, place, q)

    down_steps(0, LAG, near_step)
    got = back.at[rows(n_end, members)]
    with jax.named_scope("far"):
        pltpu.make_async_copy(got, got, far_r).wait()
    down_steps(LAG, n_pairs - 1, near_step_and_add)
    down_steps(n_pairs - 1, n_pairs, last_step)
    for i in range(n_pairs - 1 - LAG, n_pairs - 1):
        arrived_back(i)
        add_up(2 * i, 2)
        write(2 * i, 2).start()
    results_arrived(n_near, n_end, n_down - 2, 2, n_pairs - 1, mid_r, "mid")
    for q in range(2):
        results_arrived(1, n_near, n_down - 2 + q, 1, n_pairs - 1 + q, near_r, "near")
        add_up(n_down - 2 + q, 1)
        write(n_down - 2 + q, 1).start()
    with jax.named_scope("written"):
        for i in range(n_pairs - 1):
            write(2 * i, 2).wait()
        for q in range(2):
            write(n_down - 2 + q, 1).wait()
    gone = z.at[rows(n_end, members)]
    pltpu.make_async_copy(gone, gone, far_s).wait()
    gone = z.at[rows(n_near, n_end)]
    pltpu.make_async_copy(gone, gone, mid_s).wait()
    gone = z.at[rows(1, n_near)]
    pltpu.make_async_copy(gone, gone, near_s).wait()


def solution(mesh):
    members = mesh.shape["ep"]
    side = math.isqrt(members)

    def layer(x, expert, slot, gate, w_gate, w_up, w_down):
        tokens, d = x.shape[2:]
        ff, top = w_gate.shape[2], expert.shape[3]
        slots = 5 * tokens * top // (4 * members)
        total = members * slots
        n_near, n_mid, n_rest = map(len, plan(side))
        any_ = pl.BlockSpec(memory_space=pl.ANY)
        vmem = pl.BlockSpec(memory_space=pltpu.VMEM)
        turned = lambda v: v.reshape(tokens, top).T
        y = pl.pallas_call(
            functools.partial(kernel, side, slots),
            out_shape=jax.ShapeDtypeStruct((tokens, d), BF16),
            in_specs=[any_, vmem, vmem, vmem, any_, any_, any_],
            out_specs=any_,
            scratch_shapes=[
                pltpu.VMEM((total, d), BF16),
                pltpu.VMEM(((n_near + max(n_mid, n_rest)) * slots, ff), BF16),
                pltpu.VMEM((total, d), BF16),
                pltpu.VMEM((n_mid * slots, d), BF16),
                pltpu.VMEM((4 * ff, COLS), BF16),
                pltpu.VMEM((tokens, total), BF16),
                pltpu.SemaphoreType.DMA,
                pltpu.SemaphoreType.DMA((HELD + 2,)),
                pltpu.SemaphoreType.DMA,
                pltpu.SemaphoreType.DMA((members,)),
                pltpu.SemaphoreType.DMA((members,)),
                pltpu.SemaphoreType.DMA,
                pltpu.SemaphoreType.DMA,
                pltpu.SemaphoreType.DMA,
                pltpu.SemaphoreType.DMA((d // COLS,)),
                pltpu.SemaphoreType.DMA,
                pltpu.SemaphoreType.DMA((d // COLS,)),
            ],
            compiler_params=pltpu.CompilerParams(
                collective_id=0, has_side_effects=True, vmem_limit_bytes=67_043_328
            ),
            name="moe",
        )(
            x.reshape(tokens, d), turned(expert), turned(slot), turned(gate),
            w_gate.reshape(d, ff), w_up.reshape(d, ff), w_down.reshape(ff, d),
        )
        return y.reshape(1, 1, tokens, d)

    per_device, per_expert = P("dp", "ep", None, None), P("ep", None, None)
    return jax.shard_map(
        layer,
        mesh=mesh,
        in_specs=(per_device,) * 4 + (per_expert,) * 3,
        out_specs=per_device,
        check_vma=False,
    )
```
